512 devices in a mesh: gx: 64 (over z, x), gy: 8 (over y, core).
Axes of the slice: x: 4, y: 4, z: 16, core: 2. Of those that a mesh axis runs over, the one named last changes fastest.
Arguments:
- vectors: bfloat16 [65536, 768], P(('gx', 'gy')), may hold values from -6 to 6
- list_ids: int32 [65536], P(('gx', 'gy')), may hold values from 0 to 4095, as said below
- old_order: int32 [4096], replicated, may hold values from 0 to 4095, each once
- new_order: int32 [4096], replicated, may hold values from 0 to 4095, as said below
- centroids: bfloat16 [4096, 768], P('gx', 'gy'), may hold values from -6 to 6
- rotation: bfloat16 [768, 768], replicated, may hold values from -0.21875 to 0.21875
- codebook: bfloat16 [96, 8, 256], P('gy'), may hold values from -8 to 8
Outputs:
- quant_error: float32 [65536, 96], P(('gx', 'gy'))
- list_error: float32 [4096, 96], P('gx', 'gy')
The draws below stay inside these ranges and needn't reach their ends.
Inputs may be any that keep to these rules, and one draw needn't show every extreme that they name: `list_ids`: owner o holds the lists new_order[o * 64] to new_order[(o + 1) * 64 - 1]. Of the 128 vectors of one device, at most 5 name lists of one owner; in every draw some owner receives exactly 5 vectors from every device that shares its index of gy, and every device sends exactly 5 to some owner. `new_order`: each list once. `old_order`: each list once.
All inputs are finite; a program needn't handle non-finite values.
Results may differ from the reference program's by a relative error of at most 0.012.
Values may be sent and summed in bfloat16 or wider, within the bound.
A program may use at most 128 MiB of HBM per device.

```python
import jax
import jax.numpy as jnp
from jax import lax

D = 768
NLIST = 4096
M = 96
K = 256
ROWS_DEV = 128
DS = 8
LIST_OWN = 64
CAP = 5
TOKENS = 65536


def plan_slots(key):
    return jax.random.permutation(jax.random.fold_in(key, 101), NLIST).astype(jnp.int32)


def draw_new_order(key, part):
    return plan_slots(key)


def draw_list_ids(key, part):
    list_order = plan_slots(key)
    base_key = jax.random.fold_in(key, 202)
    owners = NLIST // LIST_OWN
    devices = TOKENS // ROWS_DEV
    hot_owner = jax.random.randint(jax.random.fold_in(base_key, 1), (), 0, owners)
    floor_cap = ROWS_DEV // owners + 1
    slot_owner = jnp.repeat(jnp.arange(owners, dtype=jnp.int32), CAP)
    slot_pos = jnp.tile(jnp.arange(CAP, dtype=jnp.int32), owners)

    def one_device(device):
        device_key = jax.random.fold_in(base_key, device + 7)
        key_own = jax.random.fold_in(device_key, 1)
        key_caps = jax.random.fold_in(device_key, 2)
        key_rank = jax.random.fold_in(device_key, 3)
        key_shuffle = jax.random.fold_in(device_key, 4)
        key_within = jax.random.fold_in(device_key, 5)
        own_hot = (hot_owner + 1 + jax.random.randint(key_own, (), 0, owners - 1)) % owners
        owner_caps = jax.random.randint(key_caps, (owners,), floor_cap, CAP + 1)
        owner_range = jnp.arange(owners, dtype=jnp.int32)
        is_hot = (owner_range == hot_owner) | (owner_range == own_hot)
        owner_caps = jnp.where(is_hot, CAP, owner_caps)
        is_valid = slot_pos < owner_caps[slot_owner]
        forced = is_valid & ((slot_owner == hot_owner) | (slot_owner == own_hot))
        total_slots = owners * CAP
        ranking = jax.random.permutation(key_rank, total_slots).astype(jnp.int32)
        sort_key = jnp.where(forced, ranking, jnp.where(is_valid, ranking + total_slots, ranking + 2 * total_slots))
        chosen = jnp.argsort(sort_key, stable=True)[:ROWS_DEV]
        row_owner = jax.random.permutation(key_shuffle, slot_owner[chosen])
        within = jax.random.randint(key_within, (ROWS_DEV,), 0, LIST_OWN)
        return list_order[row_owner * LIST_OWN + within]
    return jax.vmap(one_device)(jnp.arange(devices, dtype=jnp.int32)).reshape(-1).astype(jnp.int32)


def block_scale(own_key, dims, pieces, low, largest):
    factor_of, own = 1.0, jax.random.fold_in(own_key, 6)
    for axis_at, parts in pieces:
        draws = jnp.exp(jax.random.uniform(jax.random.fold_in(own, axis_at), (parts,), jnp.float32, low / len(pieces), largest / len(pieces)))
        factor_of = factor_of * jnp.repeat(draws, dims[axis_at] // parts).reshape([-1 if axis == axis_at else 1 for axis in range(len(dims))])
    return factor_of


def bell_draw(rng, shape, deviation, reach, pieces=(), kind=jnp.bfloat16):
    result = deviation * jax.random.normal(rng, shape, jnp.float32)
    if pieces:
        result = result * block_scale(rng, shape, pieces, -0.22, 0.18)
    return jnp.clip(result, -reach, reach).astype(kind)


def setup_inputs(seed: int = 0) -> dict:
    arg_keys = jax.random.split(jax.random.key(seed), 8)
    return {
        "vectors": bell_draw(arg_keys[0], (TOKENS, D), 1.0, 6.0, ((0, 512),)),
        "list_ids": draw_list_ids(jax.random.fold_in(arg_keys[7], 71), 0),
        "old_order": jax.random.permutation(arg_keys[2], NLIST).astype(jnp.int32),
        "new_order": draw_new_order(jax.random.fold_in(arg_keys[7], 71), 0),
        "centroids": bell_draw(arg_keys[4], (NLIST, D), 1.0, 6.0, ((0, 64), (1, 8))),
        "rotation": bell_draw(arg_keys[5], (D, D), D ** -0.5, 0.21875),
        "codebook": bell_draw(arg_keys[6], (M, DS, K), 1.4, 8.0, ((0, 8),)),
    }


def subspace_errors(turned, codewords, code_norm):
    row_count = turned.shape[0]
    subspaces, sub_width, code_count = codewords.shape
    group_size = 8
    group_count = subspaces // group_size
    lowered = turned.astype(jnp.bfloat16).reshape(row_count, group_count, group_size, sub_width)
    lowered = jnp.moveaxis(lowered, 1, 0)
    squares = jnp.sum((turned * turned).reshape(row_count, group_count, group_size, sub_width), axis=3)
    squares = jnp.moveaxis(squares, 1, 0)
    book_groups = codewords.reshape(group_count, group_size, sub_width, code_count)
    norm_groups = code_norm.reshape(group_count, group_size, code_count)

    def one_group(operands):
        lowered_part, square_part, book_part, norm_part = operands
        inner_terms = jnp.einsum("rgd,gdk->rgk", lowered_part.astype(jnp.float32), book_part.astype(jnp.float32), precision=lax.Precision.HIGHEST)
        inner_terms = lax.optimization_barrier(inner_terms.astype(jnp.bfloat16)).astype(jnp.float32)
        distance = square_part[:, :, None] - 2.0 * inner_terms + norm_part[None, :, :]
        return jnp.min(distance, axis=2)

    nearest = lax.map(one_group, (lowered, squares, book_groups, norm_groups))
    return jnp.moveaxis(nearest, 0, 1).reshape(row_count, subspaces)


def reference(vectors, list_ids, old_order, new_order, centroids, rotation, codebook):
    list_total = old_order.shape[0]
    slot_index = jnp.arange(list_total, dtype=jnp.int32)
    where_old = jnp.zeros((list_total,), jnp.int32).at[old_order].set(slot_index)
    list_centroid = centroids[where_old]
    rot_cent = jnp.dot(list_centroid, rotation, preferred_element_type=jnp.float32)
    code_float = codebook.astype(jnp.float32)
    code_norm = jnp.sum(code_float * code_float, axis=1)
    block_count = vectors.shape[0] // ROWS_DEV

    def one_block(operands):
        block_rows, block_labels = operands
        turned = jnp.dot(block_rows, rotation, preferred_element_type=jnp.float32) - rot_cent[block_labels]
        return subspace_errors(turned, codebook, code_norm)

    quant_error = lax.map(one_block, (vectors.reshape(block_count, ROWS_DEV, D), list_ids.reshape(block_count, ROWS_DEV)))
    quant_error = quant_error.reshape(-1, M)
    list_sums = jax.ops.segment_sum(quant_error, list_ids, num_segments=list_total)
    counts = jax.ops.segment_sum(jnp.ones(list_ids.shape, jnp.float32), list_ids, num_segments=list_total)
    average = list_sums / jnp.maximum(counts, 1.0)[:, None]
    return quant_error, average[new_order]
```

```python
import jax
import jax.numpy as jnp
from jax import lax
from jax.experimental import pallas as pl
from jax.experimental.pallas import tpu as pltpu
from jax.sharding import PartitionSpec as P

MESH = pl.DeviceIdType.MESH
F32 = jnp.float32
BF16 = jnp.bfloat16

NZ, NX, NG = 16, 4, 8
NP = NX * NG
OWN = 64
FEAT = 96
SUB = 12
ROWS = 128
CODES = 256
HOP = 4
NEAR = [4, -4, 1, -1, 2, -2, 3, -3]
FAR = [5, -5, 6, -6, 7, -7, 8]


def kernel(
    v_hbm, ids_hbm, old_hbm, new_hbm, c_hbm, r_hbm, cb_hbm,
    q_hbm, le_hbm,
    v, ids, old, new, cg, rot, cb,
    slot_out, slots, scol, y, book, wt, acc, wout, win, vr,
    qmin, tt, qt, eout, ein, zrow, bt, lm, pout, pin, qout, lout,
    in_sem, zs_sem, xs_sem, ag_sem, cbs_sem, cb_sem, sls_sem, sl_sem,
    ws_sem, w_sem, es_sem, e_sem, ps_sem, p_sem, out_sem,
):
    gx, g = lax.axis_index("gx"), lax.axis_index("gy")
    z, x = gx // NX, gx % NX
    p_me = x * NG + g

    def at_z(off):
        return lax.rem(z + (off + NZ), NZ)

    def plane_dev(p):
        return (z * NX + p // NG, p % NG)

    loads = [
        pltpu.make_async_copy(c_hbm, cg.at[gx], in_sem.at[0]),
        pltpu.make_async_copy(ids_hbm, ids, in_sem.at[1]),
        pltpu.make_async_copy(old_hbm, old, in_sem.at[2]),
        pltpu.make_async_copy(new_hbm, new, in_sem.at[3]),
        pltpu.make_async_copy(cb_hbm, cb.at[g], in_sem.at[4]),
        pltpu.make_async_copy(v_hbm, v, in_sem.at[5]),
        pltpu.make_async_copy(r_hbm, rot, in_sem.at[6]),
    ]
    for one in loads:
        one.start()

    barrier = pltpu.get_barrier_semaphore()
    for off in NEAR:
        pl.semaphore_signal(barrier, inc=1, device_id=(at_z(off) * NX + x, g), device_id_type=MESH)

    def greet(d, carry):
        pl.semaphore_signal(
            barrier, inc=1, device_id=plane_dev(lax.rem(p_me + d, NP)), device_id_type=MESH
        )
        return carry

    lax.fori_loop(1, NP, greet, 0)

    for k in (1, 2, 3):
        loads[k].wait()
    lane = lax.broadcasted_iota(jnp.int32, (ROWS, 128), 1)
    lane_f = lane.astype(F32)
    id_col = jnp.broadcast_to(ids[...].astype(F32), (ROWS, 128)).T

    def find(order, row):
        total = jnp.zeros((ROWS, 128), F32)
        for k in range(32):
            entry = jnp.broadcast_to(order[k : k + 1, :].astype(F32), (ROWS, 128))
            total = total + jnp.where(id_col == entry, lane_f + float(128 * k), 0.0)
        slot_out[row : row + 1, :] = jnp.sum(total.T, axis=0, keepdims=True)

    slot_out[...] = jnp.zeros((8, 128), F32)
    find(old, 0)
    find(new, 1)

    loads[0].wait()
    loads[4].wait()
    pl.semaphore_wait(barrier, len(NEAR) + NP - 1)

    def z_copy(block_z, to_off, k):
        block = block_z * NX + x
        return pltpu.make_async_remote_copy(
            src_ref=cg.at[block], dst_ref=cg.at[block],
            send_sem=zs_sem.at[k], recv_sem=ag_sem.at[block],
            device_id=(at_z(to_off) * NX + x, g), device_id_type=MESH,
        )

    def x_copy(block_z, d):
        block = block_z * NX + x
        return pltpu.make_async_remote_copy(
            src_ref=cg.at[block], dst_ref=cg.at[block],
            send_sem=xs_sem.at[block_z * NX + d], recv_sem=ag_sem.at[block],
            device_id=(z * NX + lax.rem(x + d, NX), g), device_id_type=MESH,
        )

    def got(block):
        pltpu.make_async_remote_copy(
            src_ref=cg.at[block], dst_ref=cg.at[block],
            send_sem=zs_sem.at[0], recv_sem=ag_sem.at[block],
            device_id=(gx, g), device_id_type=MESH,
        ).wait_recv()

    sent = []
    for k, off in enumerate(NEAR):
        sent.append(z_copy(z, off, k))
        sent[-1].start()
    for d in (1, 3, 2):
        x_copy(z, d).start()

    def slot_copy(d):
        return pltpu.make_async_remote_copy(
            src_ref=slot_out, dst_ref=slots.at[p_me],
            send_sem=sls_sem.at[d], recv_sem=sl_sem.at[p_me],
            device_id=plane_dev(lax.rem(p_me + d, NP)), device_id_type=MESH,
        )

    def send_slots(d, carry):
        slot_copy(d).start()
        return carry

    lax.fori_loop(1, NP, send_slots, 0)
    slots[p_me] = slot_out[...]

    def book_copy(d):
        return pltpu.make_async_remote_copy(
            src_ref=cb.at[g], dst_ref=cb.at[g],
            send_sem=cbs_sem.at[d], recv_sem=cb_sem.at[g],
            device_id=(gx, lax.rem(g + d, NG)), device_id_type=MESH,
        )

    for d in range(1, NG):
        book_copy(d).start()

    loads[5].wait()
    loads[6].wait()
    vr[...] = jnp.dot(v[...], rot[...], preferred_element_type=F32)

    for off in NEAR[2:]:
        got(at_z(off) * NX + x)
        for d in (1, 3, 2):
            x_copy(at_z(off), d).start()
    k = len(NEAR)
    for off in NEAR[:2]:
        got(at_z(off) * NX + x)
        step = -1 if off > 0 else 1
        for far in range(HOP if off > 0 else HOP - 1, 0, -1):
            sent.append(z_copy(at_z(off), step * far, k))
            sent[-1].start()
            k += 1
    for off in NEAR[:2]:
        for d in (1, 3, 2):
            x_copy(at_z(off), d).start()

    y[...] = jnp.zeros_like(y)
    wt[...] = jnp.zeros_like(wt)
    for q in range(NG // 2):
        for h in range(2):
            wt[q, h * 128 + FEAT : (h + 1) * 128, h * 128 : (h + 1) * 128] = jnp.ones((32, 128), BF16)

    def book_got(d):
        other = lax.rem(g + d, NG)
        pltpu.make_async_remote_copy(
            src_ref=cb.at[other], dst_ref=cb.at[other],
            send_sem=cbs_sem.at[0], recv_sem=cb_sem.at[other],
            device_id=(gx, g), device_id_type=MESH,
        ).wait_recv()

    lane_row = lax.broadcasted_iota(jnp.int32, (1, 128), 1)
    member = jnp.where(lane_row < FEAT, lane_row // 8, lax.rem(lane_row - FEAT, 16))

    for d in range(1, NG):
        book_got(d)

    def build_book(q, carry):
        for h in range(2):
            words = cb[2 * q + h].astype(F32)
            norm = jnp.sum(words * words, axis=1)
            high = norm.astype(BF16).astype(F32)
            y[0:FEAT, :] = -2.0 * words.reshape(FEAT, CODES)
            y[FEAT : FEAT + SUB, :] = high
            y[FEAT + 16 : FEAT + 16 + SUB, :] = (norm - high).astype(BF16).astype(F32)
            turned_words = y[...].T.astype(BF16)
            for i in range(SUB):
                mask = jnp.where(member == i, 1.0, 0.0).astype(BF16)
                book[q, i * CODES : (i + 1) * CODES, h * 128 : (h + 1) * 128] = turned_words * mask
        return carry

    lax.fori_loop(0, NG // 2, build_book, 0)

    for off in FAR:
        got(at_z(off) * NX + x)
        for d in (1, 3, 2):
            x_copy(at_z(off), d).start()

    def slot_got(d, carry):
        other = lax.rem(p_me + d, NP)
        pltpu.make_async_remote_copy(
            src_ref=slot_out, dst_ref=slots.at[other],
            send_sem=sls_sem.at[0], recv_sem=sl_sem.at[other],
            device_id=(gx, g), device_id_type=MESH,
        ).wait_recv()
        return carry

    lax.fori_loop(1, NP, slot_got, 0)

    def columns(j, carry):
        row = slots[x * NG + j][0:1, :]
        scol[pl.ds(pl.multiple_of(j * ROWS, ROWS), ROWS), :] = jnp.broadcast_to(row, (ROWS, 128)).T
        return carry

    lax.fori_loop(0, NG, columns, 0)
    local = lax.rem(lax.broadcasted_iota(jnp.int32, (128, 128), 0), OWN)

    def places(pp, carry):
        for h in range(2):
            at = slots[2 * pp + h][1:2, :].astype(jnp.int32)
            owner = at // OWN
            zrow[pp, :, h * 128 : (h + 1) * 128] = jnp.broadcast_to(
                jnp.where(owner % NX == x, (owner // NX).astype(F32), -1.0), (8, 128)
            )
            hit = jnp.broadcast_to(at % OWN, (128, 128)) == local
            bt[pp, :, h * 128 : (h + 1) * 128] = jnp.where(hit, 1.0, 0.0).astype(BF16)
        return carry

    lax.fori_loop(0, NP // 2, places, 0)

    lane_all = lax.broadcasted_iota(jnp.int32, (NG * ROWS, 128), 1).astype(F32)
    first = True
    for off in [0] + NEAR[2:] + NEAR[:2] + FAR:
        cz = at_z(off)
        for d in (1, 3, 2):
            got(cz * NX + lax.rem(x + d, NX))
        base = (cz * (NX * OWN)).astype(F32)
        here = scol[...] - base
        pick = jnp.concatenate(
            [jnp.where(here == lane_all + float(128 * h), 1.0, 0.0).astype(BF16) for h in range(2)],
            axis=1,
        )
        rows = cg[pl.ds(cz * NX, NX)].reshape(NX * OWN, FEAT)
        part = jnp.dot(pick, rows, preferred_element_type=F32)
        if first:
            acc[...] = part
        else:
            acc[...] += part
        first = False
    wout[...] = acc[...].astype(BF16).reshape(NG, ROWS, FEAT)

    def pick_copy(d):
        to = lax.rem(g + d, NG)
        return pltpu.make_async_remote_copy(
            src_ref=wout.at[to], dst_ref=win.at[g],
            send_sem=ws_sem.at[d], recv_sem=w_sem.at[g],
            device_id=(gx, to), device_id_type=MESH,
        )

    for d in range(1, NG):
        pick_copy(d).start()
    win[g] = wout[g]
    for d in range(1, NG):
        other = lax.rem(g + d, NG)
        pltpu.make_async_remote_copy(
            src_ref=wout.at[0], dst_ref=win.at[other],
            send_sem=ws_sem.at[0], recv_sem=w_sem.at[other],
            device_id=(gx, g), device_id_type=MESH,
        ).wait_recv()

    turned = vr[...]
    for j in range(NG):
        turned = turned - jnp.dot(
            win[j], rot[j * FEAT : (j + 1) * FEAT, :], preferred_element_type=F32
        )
    tt[...] = turned.T
    for j in range(NG):
        q, h = j // 2, j % 2
        wt[q, h * 128 : h * 128 + FEAT, h * 128 : (h + 1) * 128] = tt[
            j * FEAT : (j + 1) * FEAT, :
        ].astype(BF16)

    def search(i, carry):
        for q in range(NG // 2):
            dist = jnp.dot(
                book[q, pl.ds(pl.multiple_of(i * CODES, CODES), CODES), :], wt[q],
                preferred_element_type=F32,
            )
            low = jnp.min(dist, axis=0, keepdims=True)
            qmin[2 * q, pl.ds(i, 1), :] = low[:, :128]
            qmin[2 * q + 1, pl.ds(i, 1), :] = low[:, 128:]
        return carry

    lax.fori_loop(0, SUB, search, 0)

    qt[...] = jnp.zeros_like(qt)
    for j in range(NG):
        part = tt[j * FEAT : (j + 1) * FEAT, :].reshape(SUB, 8, ROWS)
        err = jnp.sum(part * part, axis=1) + qmin[j, 0:SUB, :]
        qt[j * SUB : (j + 1) * SUB, :] = err
        eout[j] = jnp.concatenate([err, jnp.ones((4, ROWS), F32)], axis=0).astype(BF16)

    def err_copy(d):
        to = lax.rem(p_me + d, NP)
        return pltpu.make_async_remote_copy(
            src_ref=eout.at[to % NG], dst_ref=ein.at[p_me],
            send_sem=es_sem.at[d], recv_sem=e_sem.at[p_me],
            device_id=plane_dev(to), device_id_type=MESH,
        )

    def send_err(d, carry):
        err_copy(d).start()
        return carry

    lax.fori_loop(1, NP, send_err, 0)
    ein[p_me] = eout[g]

    qout[...] = qt[...].T[:, : NG * SUB]
    q_store = pltpu.make_async_copy(qout, q_hbm, out_sem.at[0])
    q_store.start()

    def err_got(d, carry):
        other = lax.rem(p_me + d, NP)
        pltpu.make_async_remote_copy(
            src_ref=eout.at[0], dst_ref=ein.at[other],
            send_sem=es_sem.at[0], recv_sem=e_sem.at[other],
            device_id=(gx, g), device_id_type=MESH,
        ).wait_recv()
        return carry

    lax.fori_loop(1, NP, err_got, 0)

    def sums(pp, total):
        for h in range(2):
            err = ein[2 * pp + h].astype(F32)
            owner = zrow[pp, 0:1, h * 128 : (h + 1) * 128]
            for a in range(NZ):
                lm[a * 16 : (a + 1) * 16, h * 128 : (h + 1) * 128] = jnp.where(
                    owner == float(a), err, 0.0
                ).astype(BF16)
        return total + lax.dot_general(
            lm[...], bt[pp], (((1,), (1,)), ((), ())), preferred_element_type=F32
        )

    total = lax.fori_loop(0, NP // 2, sums, jnp.zeros((NZ * 16, 128), F32))
    lane8 = lax.broadcasted_iota(jnp.int32, (8, 128), 1)
    for a in range(NZ):
        pout[a] = jnp.where(lane8 < OWN, total[a * 16 : a * 16 + 8, :], total[a * 16 + 8 : a * 16 + 16, :])

    def sum_copy(d):
        to = at_z(d)
        return pltpu.make_async_remote_copy(
            src_ref=pout.at[to], dst_ref=pin.at[z],
            send_sem=ps_sem.at[d], recv_sem=p_sem.at[z],
            device_id=(to * NX + x, g), device_id_type=MESH,
        )

    for d in range(1, NZ):
        sum_copy(d).start()
    pin[z] = pout[z]
    for d in range(1, NZ):
        other = at_z(d)
        pltpu.make_async_remote_copy(
            src_ref=pout.at[0], dst_ref=pin.at[other],
            send_sem=ps_sem.at[0], recv_sem=p_sem.at[other],
            device_id=(gx, g), device_id_type=MESH,
        ).wait_recv()
    whole = jnp.sum(pin[...], axis=0)
    count = jnp.broadcast_to(whole[4:5, :], (8, 128))
    count = jnp.where(lane8 < OWN, pltpu.roll(count, OWN, 1), count)
    mean = (whole / jnp.maximum(count, 1.0)).T
    lout[:, 0:8] = mean[0:OWN, :]
    lout[:, 8:SUB] = mean[OWN : 2 * OWN, 0 : SUB - 8]
    l_store = pltpu.make_async_copy(lout, le_hbm, out_sem.at[1])
    l_store.start()

    for one in sent:
        one.wait_send()

    def x_done(bz, carry):
        for d in range(1, NX):
            x_copy(bz, d).wait_send()
        return carry

    lax.fori_loop(0, NZ, x_done, 0)
    for d in range(1, NG):
        book_copy(d).wait_send()
        pick_copy(d).wait_send()

    def plane_done(d, carry):
        slot_copy(d).wait_send()
        err_copy(d).wait_send()
        return carry

    lax.fori_loop(1, NP, plane_done, 0)
    for d in range(1, NZ):
        sum_copy(d).wait_send()
    q_store.wait()
    l_store.wait()


def on_device(vectors, list_ids, old_order, new_order, centroids, rotation, codebook):
    dma = pltpu.SemaphoreType.DMA
    any_spec = pl.BlockSpec(memory_space=pl.ANY)
    return pl.pallas_call(
        kernel,
        out_shape=(
            jax.ShapeDtypeStruct((ROWS, NG * SUB), F32),
            jax.ShapeDtypeStruct((OWN, SUB), F32),
        ),
        in_specs=[any_spec] * 7,
        out_specs=(any_spec, any_spec),
        scratch_shapes=[
            pltpu.VMEM((ROWS, 768), BF16),
            pltpu.VMEM((1, 128), jnp.int32),
            pltpu.VMEM((32, 128), jnp.int32),
            pltpu.VMEM((32, 128), jnp.int32),
            pltpu.VMEM((NZ * NX, OWN, FEAT), BF16),
            pltpu.VMEM((768, 768), BF16),
            pltpu.VMEM((NG, SUB, 8, CODES), BF16),
            pltpu.VMEM((8, 128), F32),
            pltpu.VMEM((NP, 8, 128), F32),
            pltpu.VMEM((NG * ROWS, 128), F32),
            pltpu.VMEM((128, CODES), F32),
            pltpu.VMEM((NG // 2, SUB * CODES, 256), BF16),
            pltpu.VMEM((NG // 2, 256, 256), BF16),
            pltpu.VMEM((NG * ROWS, FEAT), F32),
            pltpu.VMEM((NG, ROWS, FEAT), BF16),
            pltpu.VMEM((NG, ROWS, FEAT), BF16),
            pltpu.VMEM((ROWS, 768), F32),
            pltpu.VMEM((NG, 16, ROWS), F32),
            pltpu.VMEM((768, ROWS), F32),
            pltpu.VMEM((128, ROWS), F32),
            pltpu.VMEM((NG, 16, ROWS), BF16),
            pltpu.VMEM((NP, 16, ROWS), BF16),
            pltpu.VMEM((NP // 2, 8, 256), F32),
            pltpu.VMEM((NP // 2, 128, 256), BF16),
            pltpu.VMEM((NZ * 16, 256), BF16),
            pltpu.VMEM((NZ, 8, 128), F32),
            pltpu.VMEM((NZ, 8, 128), F32),
            pltpu.VMEM((ROWS, NG * SUB), F32),
            pltpu.VMEM((OWN, SUB), F32),
            dma((7,)),
            dma((NZ,)),
            dma((NZ * NX,)),
            dma((NZ * NX,)),
            dma((NG,)),
            dma((NG,)),
            dma((NP,)),
            dma((NP,)),
            dma((NG,)),
            dma((NG,)),
            dma((NP,)),
            dma((NP,)),
            dma((NZ,)),
            dma((NZ,)),
            dma((2,)),
        ],
        compiler_params=pltpu.CompilerParams(
            collective_id=0, has_side_effects=True, vmem_limit_bytes=48 * 1024 * 1024
        ),
    )(
        vectors,
        list_ids.reshape(1, ROWS),
        old_order.reshape(32, 128),
        new_order.reshape(32, 128),
        centroids,
        rotation,
        codebook,
    )


def solution(mesh):
    both = ("gx", "gy")
    in_specs = (P(both, None), P(both), P(), P(), P("gx", "gy"), P(), P("gy", None, None))
    out_specs = (P(both, None), P("gx", "gy"))
    return jax.shard_map(
        on_device, mesh=mesh, in_specs=in_specs, out_specs=out_specs, check_vma=False
    )
```

```python
import jax
import jax.numpy as jnp
from jax import lax
from jax.experimental import pallas as pl
from jax.experimental.pallas import tpu as pltpu
from jax.sharding import PartitionSpec as P

MESH = pl.DeviceIdType.MESH
F32 = jnp.float32
BF16 = jnp.bfloat16

NZ, NX, NG = 16, 4, 8
NP = NX * NG
OWN = 64
FEAT = 96
SUB = 12
ROWS = 128
CODES = 256
CHUNK = 256
WIDE = 6
HOP = 4
NEAR = [4, -4, 1, -1, 2, -2, 3, -3]
FAR = [5, -5, 6, -6, 7, -7, 8]


def kernel(
    v_hbm, ids_hbm, old_hbm, new_hbm, c_hbm, r_hbm, cb_hbm,
    q_hbm, le_hbm,
    v, ids, old, new, cg, rot, cb,
    slot_out, slots, high, low_hot, y, book, wt, acc, wout, win, vr,
    qmin, tt, qt, eout, ein, zrow, bt, lm, pout, pin, lout,
    in_sem, zs_sem, xs_sem, ag_sem, cbs_sem, cb_sem, sls_sem, sl_sem,
    ws_sem, w_sem, es_sem, e_sem, ps_sem, p_sem, out_sem,
):
    gx, g = lax.axis_index("gx"), lax.axis_index("gy")
    z, x = gx // NX, gx % NX
    p_me = x * NG + g

    def at_z(off):
        return lax.rem(z + (off + NZ), NZ)

    def plane_dev(p):
        return (z * NX + p // NG, p % NG)

    loads = [
        pltpu.make_async_copy(c_hbm, cg.at[gx], in_sem.at[0]),
        pltpu.make_async_copy(ids_hbm, ids, in_sem.at[1]),
        pltpu.make_async_copy(old_hbm, old, in_sem.at[2]),
        pltpu.make_async_copy(new_hbm, new, in_sem.at[3]),
        pltpu.make_async_copy(cb_hbm, cb.at[g], in_sem.at[4]),
        pltpu.make_async_copy(v_hbm, v, in_sem.at[5]),
        pltpu.make_async_copy(r_hbm, rot, in_sem.at[6]),
    ]
    for one in loads:
        one.start()

    barrier = pltpu.get_barrier_semaphore()
    for off in NEAR:
        pl.semaphore_signal(barrier, inc=1, device_id=(at_z(off) * NX + x, g), device_id_type=MESH)

    def greet(d, carry):
        pl.semaphore_signal(
            barrier, inc=1, device_id=plane_dev(lax.rem(p_me + d, NP)), device_id_type=MESH
        )
        return carry

    lax.fori_loop(1, NP, greet, 0)

    for k in (1, 2, 3):
        loads[k].wait()
    lane = lax.broadcasted_iota(jnp.int32, (ROWS, 128), 1)
    lane_f = lane.astype(F32)
    id_col = jnp.broadcast_to(ids[...].astype(F32), (ROWS, 128)).T

    def find(order, row):
        total = jnp.zeros((ROWS, 128), F32)
        for k in range(32):
            entry = jnp.broadcast_to(order[k : k + 1, :].astype(F32), (ROWS, 128))
            total = total + jnp.where(id_col == entry, lane_f + float(128 * k), 0.0)
        slot_out[row : row + 1, :] = jnp.sum(total.T, axis=0, keepdims=True)

    find(old, 0)
    find(new, 1)

    loads[0].wait()
    loads[4].wait()
    pl.semaphore_wait(barrier, len(NEAR) + NP - 1)

    def z_copy(block_z, to_off, k):
        block = block_z * NX + x
        return pltpu.make_async_remote_copy(
            src_ref=cg.at[block], dst_ref=cg.at[block],
            send_sem=zs_sem.at[k], recv_sem=ag_sem.at[block],
            device_id=(at_z(to_off) * NX + x, g), device_id_type=MESH,
        )

    def x_copy(block_z, d):
        block = block_z * NX + x
        return pltpu.make_async_remote_copy(
            src_ref=cg.at[block], dst_ref=cg.at[block],
            send_sem=xs_sem.at[block_z * NX + d], recv_sem=ag_sem.at[block],
            device_id=(z * NX + lax.rem(x + d, NX), g), device_id_type=MESH,
        )

    def got(block):
        pltpu.make_async_remote_copy(
            src_ref=cg.at[block], dst_ref=cg.at[block],
            send_sem=zs_sem.at[0], recv_sem=ag_sem.at[block],
            device_id=(gx, g), device_id_type=MESH,
        ).wait_recv()

    sent = []
    for k, off in enumerate(NEAR):
        sent.append(z_copy(z, off, k))
        sent[-1].start()
    for d in (1, 3, 2):
        x_copy(z, d).start()

    def slot_copy(d):
        return pltpu.make_async_remote_copy(
            src_ref=slot_out, dst_ref=slots.at[p_me],
            send_sem=sls_sem.at[d], recv_sem=sl_sem.at[p_me],
            device_id=plane_dev(lax.rem(p_me + d, NP)), device_id_type=MESH,
        )

    def send_slots(d, carry):
        slot_copy(d).start()
        return carry

    lax.fori_loop(1, NP, send_slots, 0)
    slots[p_me] = slot_out[...]

    def book_copy(d):
        return pltpu.make_async_remote_copy(
            src_ref=cb.at[g], dst_ref=cb.at[g],
            send_sem=cbs_sem.at[d], recv_sem=cb_sem.at[g],
            device_id=(gx, lax.rem(g + d, NG)), device_id_type=MESH,
        )

    for d in range(1, NG):
        book_copy(d).start()

    loads[5].wait()
    loads[6].wait()
    vr[...] = jnp.dot(v[...], rot[...], preferred_element_type=F32)

    def spread(off):
        for d in (1, 3, 2):
            x_copy(at_z(off), d).start()

    for off in NEAR[2:6]:
        got(at_z(off) * NX + x)
        spread(off)
    k = len(NEAR)
    for off in NEAR[:2]:
        got(at_z(off) * NX + x)
        step = -1 if off > 0 else 1
        for far in range(HOP if off > 0 else HOP - 1, 0, -1):
            sent.append(z_copy(at_z(off), step * far, k))
            sent[-1].start()
            k += 1
    for off in NEAR[6:] + NEAR[:2]:
        if abs(off) < HOP:
            got(at_z(off) * NX + x)
        spread(off)

    y[...] = jnp.zeros_like(y)
    wt[...] = jnp.zeros_like(wt)
    for q in range(NG // 2):
        for h in range(2):
            wt[q, h * 128 + FEAT : (h + 1) * 128, h * 128 : (h + 1) * 128] = jnp.ones((32, 128), BF16)

    def book_got(d):
        other = lax.rem(g + d, NG)
        pltpu.make_async_remote_copy(
            src_ref=cb.at[other], dst_ref=cb.at[other],
            send_sem=cbs_sem.at[0], recv_sem=cb_sem.at[other],
            device_id=(gx, g), device_id_type=MESH,
        ).wait_recv()

    lane_row = lax.broadcasted_iota(jnp.int32, (1, 128), 1)
    member = jnp.where(lane_row < FEAT, lane_row // 8, lax.rem(lane_row - FEAT, 16))

    for d in range(1, NG):
        book_got(d)

    def build_book(q, carry):
        for h in range(2):
            words = cb[2 * q + h].astype(F32)
            norm = jnp.sum(words * words, axis=1)
            high = norm.astype(BF16).astype(F32)
            y[0:FEAT, :] = -2.0 * words.reshape(FEAT, CODES)
            y[FEAT : FEAT + SUB, :] = high
            y[FEAT + 16 : FEAT + 16 + SUB, :] = (norm - high).astype(BF16).astype(F32)
            turned_words = y[...].T.astype(BF16)
            for i in range(SUB):
                mask = jnp.where(member == i, 1.0, 0.0).astype(BF16)
                book[q, i * CODES : (i + 1) * CODES, h * 128 : (h + 1) * 128] = turned_words * mask
        return carry

    lax.fori_loop(0, NG // 2, build_book, 0)

    def slot_got(d, carry):
        other = lax.rem(p_me + d, NP)
        pltpu.make_async_remote_copy(
            src_ref=slot_out, dst_ref=slots.at[other],
            send_sem=sls_sem.at[0], recv_sem=sl_sem.at[other],
            device_id=(gx, g), device_id_type=MESH,
        ).wait_recv()
        return carry

    lax.fori_loop(1, NP, slot_got, 0)

    def columns(j, carry):
        row = slots[x * NG + j][0:1, :].astype(jnp.int32)
        at = pl.ds(pl.multiple_of(j * ROWS, ROWS), ROWS)
        high[at, :] = jnp.broadcast_to((row // CHUNK).astype(F32), (ROWS, 128)).T
        rest = jnp.broadcast_to((row % CHUNK).astype(F32), (ROWS, 128)).T
        for h in range(2):
            low_hot[at, h * 128 : (h + 1) * 128] = jnp.where(
                rest == lane_f + float(128 * h), 1.0, 0.0
            ).astype(BF16)
        return carry

    lax.fori_loop(0, NG, columns, 0)
    local = lax.rem(lax.broadcasted_iota(jnp.int32, (128, 128), 0), OWN)

    def places(pp, carry):
        for h in range(2):
            at = slots[2 * pp + h][1:2, :].astype(jnp.int32)
            owner = at // OWN
            zrow[pp, :, h * 128 : (h + 1) * 128] = jnp.broadcast_to(
                jnp.where(owner % NX == x, (owner // NX).astype(F32), -1.0), (8, 128)
            )
            hit = jnp.broadcast_to(at % OWN, (128, 128)) == local
            bt[pp, :, h * 128 : (h + 1) * 128] = jnp.where(hit, 1.0, 0.0).astype(BF16)
        return carry

    for off in FAR:
        got(at_z(off) * NX + x)
        spread(off)

    lax.fori_loop(0, NP // 2, places, 0)

    acc[...] = jnp.zeros_like(acc)
    blank = jnp.zeros((CHUNK, 128 - FEAT), BF16)

    def pick(offs):
        sides = []
        for off in offs:
            cz = at_z(off)
            for d in (1, 3, 2):
                got(cz * NX + lax.rem(x + d, NX))
            rows = cg[pl.ds(cz * NX, NX)].reshape(CHUNK, FEAT)
            sides.append(jnp.concatenate([rows, blank], axis=1))
        both = jnp.concatenate(sides, axis=1)
        za, zb = (at_z(off).astype(F32) for off in offs)
        part = jnp.dot(low_hot[...], both, preferred_element_type=F32)
        acc[...] = jnp.where(
            high[...] == za, part[:, :128], jnp.where(high[...] == zb, part[:, 128:], acc[...])
        )

    order = [0, 1, -1, 2, -2, 3, -3, 4, -4] + FAR
    for k in range(0, NZ, 2):
        if k == 8:
            pass
        pick(order[k : k + 2])
    wout[...] = acc[:, :FEAT].astype(BF16).reshape(NG, ROWS, FEAT)

    def pick_copy(d):
        to = lax.rem(g + d, NG)
        return pltpu.make_async_remote_copy(
            src_ref=wout.at[to], dst_ref=win.at[g],
            send_sem=ws_sem.at[d], recv_sem=w_sem.at[g],
            device_id=(gx, to), device_id_type=MESH,
        )

    for d in range(1, NG):
        pick_copy(d).start()
    win[g] = wout[g]
    for d in range(1, NG):
        other = lax.rem(g + d, NG)
        pltpu.make_async_remote_copy(
            src_ref=wout.at[0], dst_ref=win.at[other],
            send_sem=ws_sem.at[0], recv_sem=w_sem.at[other],
            device_id=(gx, g), device_id_type=MESH,
        ).wait_recv()

    turned = vr[...]
    for j in range(NG):
        turned = turned - jnp.dot(
            win[j], rot[j * FEAT : (j + 1) * FEAT, :], preferred_element_type=F32
        )
    tt[...] = turned.T
    for j in range(NG):
        q, h = j // 2, j % 2
        wt[q, h * 128 : h * 128 + FEAT, h * 128 : (h + 1) * 128] = tt[
            j * FEAT : (j + 1) * FEAT, :
        ].astype(BF16)

    for q in range(NG // 2):
        for i in range(0, SUB, WIDE):
            dist = jnp.dot(
                book[q, i * CODES : (i + WIDE) * CODES, :], wt[q], preferred_element_type=F32
            )
            low = jnp.min(dist.reshape(WIDE, CODES, 256), axis=1)
            qmin[2 * q, i : i + WIDE, :] = low[:, :128]
            qmin[2 * q + 1, i : i + WIDE, :] = low[:, 128:]

    for j in range(NG):
        part = tt[j * FEAT : (j + 1) * FEAT, :].reshape(SUB, 8, ROWS)
        err = jnp.sum(part * part, axis=1) + qmin[j, 0:SUB, :]
        qt[j * SUB : (j + 1) * SUB, :] = err
        eout[j] = jnp.concatenate([err, jnp.ones((4, ROWS), F32)], axis=0).astype(BF16)

    def err_copy(d):
        to = lax.rem(p_me + d, NP)
        return pltpu.make_async_remote_copy(
            src_ref=eout.at[to % NG], dst_ref=ein.at[p_me],
            send_sem=es_sem.at[d], recv_sem=e_sem.at[p_me],
            device_id=plane_dev(to), device_id_type=MESH,
        )

    def send_err(d, carry):
        err_copy(d).start()
        return carry

    lax.fori_loop(1, NP, send_err, 0)
    ein[p_me] = eout[g]

    q_store = pltpu.make_async_copy(qt, q_hbm, out_sem.at[0])
    q_store.start()

    def err_got(d, carry):
        other = lax.rem(p_me + d, NP)
        pltpu.make_async_remote_copy(
            src_ref=eout.at[0], dst_ref=ein.at[other],
            send_sem=es_sem.at[0], recv_sem=e_sem.at[other],
            device_id=(gx, g), device_id_type=MESH,
        ).wait_recv()
        return carry

    lax.fori_loop(1, NP, err_got, 0)

    def sums(pp, total):
        for h in range(2):
            err = ein[2 * pp + h].astype(F32)
            owner = zrow[pp, 0:1, h * 128 : (h + 1) * 128]
            for a in range(NZ):
                lm[pp, a * 16 : (a + 1) * 16, h * 128 : (h + 1) * 128] = jnp.where(
                    owner == float(a), err, 0.0
                ).astype(BF16)
        return total + lax.dot_general(
            lm[pp], bt[pp], (((1,), (1,)), ((), ())), preferred_element_type=F32
        )

    total = jnp.zeros((NZ * 16, 128), F32)
    for pp in range(NP // 2):
        total = sums(pp, total)
    lane8 = lax.broadcasted_iota(jnp.int32, (8, 128), 1)
    for a in range(NZ):
        pout[a] = jnp.where(lane8 < OWN, total[a * 16 : a * 16 + 8, :], total[a * 16 + 8 : a * 16 + 16, :])

    def sum_copy(d):
        to = at_z(d)
        return pltpu.make_async_remote_copy(
            src_ref=pout.at[to], dst_ref=pin.at[z],
            send_sem=ps_sem.at[d], recv_sem=p_sem.at[z],
            device_id=(to * NX + x, g), device_id_type=MESH,
        )

    for d in range(1, NZ):
        sum_copy(d).start()
    pin[z] = pout[z]
    for d in range(1, NZ):
        other = at_z(d)
        pltpu.make_async_remote_copy(
            src_ref=pout.at[0], dst_ref=pin.at[other],
            send_sem=ps_sem.at[0], recv_sem=p_sem.at[other],
            device_id=(gx, g), device_id_type=MESH,
        ).wait_recv()
    whole = jnp.sum(pin[...], axis=0)
    count = jnp.broadcast_to(whole[4:5, :], (8, 128))
    count = jnp.where(lane8 < OWN, pltpu.roll(count, OWN, 1), count)
    mean = whole / jnp.maximum(count, 1.0)
    lout[0:8, :] = mean[:, :OWN]
    lout[8:SUB, :] = pltpu.roll(mean, OWN, 1)[: SUB - 8, :OWN]
    l_store = pltpu.make_async_copy(lout, le_hbm, out_sem.at[1])
    l_store.start()

    for one in sent:
        one.wait_send()

    def x_done(bz, carry):
        for d in range(1, NX):
            x_copy(bz, d).wait_send()
        return carry

    lax.fori_loop(0, NZ, x_done, 0)
    for d in range(1, NG):
        book_copy(d).wait_send()
        pick_copy(d).wait_send()

    def plane_done(d, carry):
        slot_copy(d).wait_send()
        err_copy(d).wait_send()
        return carry

    lax.fori_loop(1, NP, plane_done, 0)
    for d in range(1, NZ):
        sum_copy(d).wait_send()
    q_store.wait()
    l_store.wait()


def on_device(vectors, list_ids, old_order, new_order, centroids, rotation, codebook):
    dma = pltpu.SemaphoreType.DMA
    any_spec = pl.BlockSpec(memory_space=pltpu.HBM)
    errors, means = pl.pallas_call(
        kernel,
        out_shape=(
            jax.ShapeDtypeStruct((NG * SUB, ROWS), F32),
            jax.ShapeDtypeStruct((SUB, OWN), F32),
        ),
        in_specs=[any_spec] * 7,
        out_specs=(any_spec, any_spec),
        scratch_shapes=[
            pltpu.VMEM((ROWS, 768), BF16),
            pltpu.VMEM((1, 128), jnp.int32),
            pltpu.VMEM((32, 128), jnp.int32),
            pltpu.VMEM((32, 128), jnp.int32),
            pltpu.VMEM((NZ * NX, OWN, FEAT), BF16),
            pltpu.VMEM((768, 768), BF16),
            pltpu.VMEM((NG, SUB, 8, CODES), BF16),
            pltpu.VMEM((2, 128), F32),
            pltpu.VMEM((NP, 2, 128), F32),
            pltpu.VMEM((NG * ROWS, 128), F32),
            pltpu.VMEM((NG * ROWS, 256), BF16),
            pltpu.VMEM((128, CODES), F32),
            pltpu.VMEM((NG // 2, SUB * CODES, 256), BF16),
            pltpu.VMEM((NG // 2, 256, 256), BF16),
            pltpu.VMEM((NG * ROWS, 128), F32),
            pltpu.VMEM((NG, ROWS, FEAT), BF16),
            pltpu.VMEM((NG, ROWS, FEAT), BF16),
            pltpu.VMEM((ROWS, 768), F32),
            pltpu.VMEM((NG, 16, ROWS), F32),
            pltpu.VMEM((768, ROWS), F32),
            pltpu.VMEM((NG * SUB, ROWS), F32),
            pltpu.VMEM((NG, 16, ROWS), BF16),
            pltpu.VMEM((NP, 16, ROWS), BF16),
            pltpu.VMEM((NP // 2, 8, 256), F32),
            pltpu.VMEM((NP // 2, 128, 256), BF16),
            pltpu.VMEM((NP // 2, NZ * 16, 256), BF16),
            pltpu.VMEM((NZ, 8, 128), F32),
            pltpu.VMEM((NZ, 8, 128), F32),
            pltpu.VMEM((SUB, OWN), F32),
            dma((7,)),
            dma((NZ,)),
            dma((NZ * NX,)),
            dma((NZ * NX,)),
            dma((NG,)),
            dma((NG,)),
            dma((NP,)),
            dma((NP,)),
            dma((NG,)),
            dma((NG,)),
            dma((NP,)),
            dma((NP,)),
            dma((NZ,)),
            dma((NZ,)),
            dma((2,)),
        ],
        compiler_params=pltpu.CompilerParams(
            collective_id=0, has_side_effects=True, vmem_limit_bytes=67043328
        ),
    )(
        vectors,
        list_ids.reshape(1, ROWS),
        old_order.reshape(32, 128),
        new_order.reshape(32, 128),
        centroids,
        rotation,
        codebook,
    )
    return errors.T, means.T


def solution(mesh):
    both = ("gx", "gy")
    in_specs = (P(both, None), P(both), P(), P(), P("gx", "gy"), P(), P("gy", None, None))
    out_specs = (P(both, None), P("gx", "gy"))
    return jax.shard_map(
        on_device, mesh=mesh, in_specs=in_specs, out_specs=out_specs, check_vma=False
    )
```

```python
import itertools

import jax
import jax.numpy as jnp
from jax import lax
from jax.experimental import pallas as pl
from jax.experimental.pallas import tpu as pltpu
from jax.sharding import PartitionSpec as P

MESH = pl.DeviceIdType.MESH
F32 = jnp.float32
BF16 = jnp.bfloat16

NZ, NX, NG = 16, 4, 8
NP = NX * NG
OWN = 64
FEAT = 96
SUB = 12
ROWS = 128
CODES = 256
CHUNK = 256
PACKED = OWN * FEAT // 128
WIDE = 6
HOP = 4
NEAR = [4, -4, 1, -1, 2, -2, 3, -3]
FAR = [5, -5, 6, -6, 7, -7, 8]


def kernel(
    v_hbm, ids_hbm, old_hbm, new_hbm, c_hbm, r_hbm, cb_hbm,
    q_hbm, le_hbm,
    v, ids, old, new, block_in, cg, rot, cb,
    slot_out, slots, high, low_hot, y, book, wt, acc, wout, win, vr,
    qmin, tt, qt, eout, ein, zrow, bt, lm, pout, pin, lout,
    in_sem, zs_sem, xs_sem, ag_sem, cbs_sem, cb_sem, sls_sem, sl_sem,
    ws_sem, w_sem, es_sem, e_sem, ps_sem, p_sem, out_sem,
):
    gx, g = lax.axis_index("gx"), lax.axis_index("gy")
    z, x = gx // NX, gx % NX
    p_me = x * NG + g

    def at_z(off):
        return lax.rem(z + (off + NZ), NZ)

    x_to = [lax.rem(x + d, NX) for d in range(NX)]
    g_to = [lax.rem(g + d, NG) for d in range(NG)]
    gx_to = [z * NX + one for one in x_to]
    plane = [(dx, dg) for dx in (2, 1, 3, 0) for dg in (4, 5, 2, 3, 6, 7, 1, 0) if dx or dg]

    loads = [
        pltpu.make_async_copy(c_hbm, block_in, in_sem.at[0]),
        pltpu.make_async_copy(ids_hbm, ids, in_sem.at[1]),
        pltpu.make_async_copy(old_hbm, old, in_sem.at[2]),
        pltpu.make_async_copy(new_hbm, new, in_sem.at[3]),
        pltpu.make_async_copy(cb_hbm, cb.at[g], in_sem.at[4]),
        pltpu.make_async_copy(v_hbm, v, in_sem.at[5]),
        pltpu.make_async_copy(r_hbm, rot, in_sem.at[6]),
    ]
    for one in loads:
        one.start()

    barrier = pltpu.get_barrier_semaphore()
    for off in NEAR:
        pl.semaphore_signal(barrier, inc=1, device_id=(at_z(off) * NX + x, g), device_id_type=MESH)

    for dx, dg in plane:
        pl.semaphore_signal(barrier, inc=1, device_id=(gx_to[dx], g_to[dg]), device_id_type=MESH)

    loads[0].wait()
    for k in range(3):
        tail = block_in[48:64, 32 * k : 32 * (k + 1)]
        cg[gx, 16 * k : 16 * (k + 1), :] = jnp.concatenate(
            [block_in[16 * k : 16 * (k + 1), :], tail], axis=1
        )
    pl.semaphore_wait(barrier, len(NEAR) + NP - 1)

    def z_copy(block_z, to_off, k):
        block = block_z * NX + x
        return pltpu.make_async_remote_copy(
            src_ref=cg.at[block], dst_ref=cg.at[block],
            send_sem=zs_sem.at[k], recv_sem=ag_sem.at[block],
            device_id=(at_z(to_off) * NX + x, g), device_id_type=MESH,
        )

    def x_copy(block_z, d):
        block = block_z * NX + x
        return pltpu.make_async_remote_copy(
            src_ref=cg.at[block], dst_ref=cg.at[block],
            send_sem=xs_sem.at[block_z * NX + d], recv_sem=ag_sem.at[block],
            device_id=(z * NX + lax.rem(x + d, NX), g), device_id_type=MESH,
        )

    def got(block):
        pltpu.make_async_remote_copy(
            src_ref=cg.at[block], dst_ref=cg.at[block],
            send_sem=zs_sem.at[0], recv_sem=ag_sem.at[block],
            device_id=(gx, g), device_id_type=MESH,
        ).wait_recv()

    sent = []
    for k, off in enumerate(NEAR):
        sent.append(z_copy(z, off, k))
        sent[-1].start()
    for d in (1, 3, 2):
        x_copy(z, d).start()

    for k in (1, 2, 3):
        loads[k].wait()
    lane = lax.broadcasted_iota(jnp.int32, (ROWS, 128), 1)
    lane_f = lane.astype(F32)
    id_col = jnp.broadcast_to(ids[...].astype(F32), (ROWS, 128)).T

    def find(order, row):
        total = jnp.zeros((ROWS, 128), F32)
        for k in range(32):
            entry = jnp.broadcast_to(order[k : k + 1, :].astype(F32), (ROWS, 128))
            total = total + jnp.where(id_col == entry, lane_f + float(128 * k), 0.0)
        slot_out[row : row + 1, :] = jnp.sum(total.T, axis=0, keepdims=True)

    find(old, 0)
    find(new, 1)

    def slot_copy(dx, dg):
        return pltpu.make_async_remote_copy(
            src_ref=slot_out, dst_ref=slots.at[p_me],
            send_sem=sls_sem.at[dx * NG + dg], recv_sem=sl_sem.at[p_me],
            device_id=(gx_to[dx], g_to[dg]), device_id_type=MESH,
        )

    for dx, dg in plane:
        slot_copy(dx, dg).start()
    slots[p_me] = slot_out[...]

    def book_copy(d):
        return pltpu.make_async_remote_copy(
            src_ref=cb.at[g], dst_ref=cb.at[g],
            send_sem=cbs_sem.at[d], recv_sem=cb_sem.at[g],
            device_id=(gx, lax.rem(g + d, NG)), device_id_type=MESH,
        )

    loads[4].wait()
    for d in range(1, NG):
        book_copy(d).start()

    loads[5].wait()
    loads[6].wait()
    vr[...] = jnp.dot(v[...], rot[...], preferred_element_type=F32)

    def spread(off):
        for d in (1, 3, 2):
            x_copy(at_z(off), d).start()

    for off in NEAR[2:6]:
        got(at_z(off) * NX + x)
        spread(off)
    k = len(NEAR)
    for off in NEAR[:2]:
        got(at_z(off) * NX + x)
        step = -1 if off > 0 else 1
        for far in range(HOP if off > 0 else HOP - 1, 0, -1):
            sent.append(z_copy(at_z(off), step * far, k))
            sent[-1].start()
            k += 1
    for off in NEAR[6:] + NEAR[:2]:
        if abs(off) < HOP:
            got(at_z(off) * NX + x)
        spread(off)

    y[...] = jnp.zeros_like(y)
    wt[...] = jnp.zeros_like(wt)
    for q in range(NG // 2):
        for h in range(2):
            wt[q, h * 128 + FEAT : (h + 1) * 128, h * 128 : (h + 1) * 128] = jnp.ones((32, 128), BF16)

    def book_got(d):
        other = lax.rem(g + d, NG)
        pltpu.make_async_remote_copy(
            src_ref=cb.at[other], dst_ref=cb.at[other],
            send_sem=cbs_sem.at[0], recv_sem=cb_sem.at[other],
            device_id=(gx, g), device_id_type=MESH,
        ).wait_recv()

    lane_row = lax.broadcasted_iota(jnp.int32, (1, 128), 1)
    member = jnp.where(lane_row < FEAT, lane_row // 8, lax.rem(lane_row - FEAT, 16))

    def build_book(q, carry):
        for h in range(2):
            words = cb[2 * q + h].astype(F32)
            norm = jnp.sum(words * words, axis=1)
            high = norm.astype(BF16).astype(F32)
            y[0:FEAT, :] = -2.0 * words.reshape(FEAT, CODES)
            y[FEAT : FEAT + SUB, :] = high
            y[FEAT + 16 : FEAT + 16 + SUB, :] = (norm - high).astype(BF16).astype(F32)
            turned_words = y[...].T.astype(BF16)
            for i in range(SUB):
                mask = jnp.where(member == i, 1.0, 0.0).astype(BF16)
                book[q, i * CODES : (i + 1) * CODES, h * 128 : (h + 1) * 128] = turned_words * mask
        return carry


    def slot_got(d, carry):
        other = lax.rem(p_me + d, NP)
        pltpu.make_async_remote_copy(
            src_ref=slot_out, dst_ref=slots.at[other],
            send_sem=sls_sem.at[0], recv_sem=sl_sem.at[other],
            device_id=(gx, g), device_id_type=MESH,
        ).wait_recv()
        return carry

    lax.fori_loop(1, NP, slot_got, 0)

    def columns(j, carry):
        row = slots[x * NG + j][0:1, :].astype(jnp.int32)
        at = pl.ds(pl.multiple_of(j * ROWS, ROWS), ROWS)
        high[at, :] = jnp.broadcast_to((row // CHUNK).astype(F32), (ROWS, 128)).T
        inner = row % CHUNK
        block, spot = inner // OWN, inner % OWN
        place = jnp.where(spot < 48, block * 48 + spot, 144 + block * 16 + spot)
        rest = jnp.broadcast_to(place.astype(F32), (ROWS, 128)).T
        for h in range(2):
            low_hot[at, h * 128 : (h + 1) * 128] = jnp.where(
                rest == lane_f + float(128 * h), -1.0, 0.0
            ).astype(BF16)
        return carry

    lax.fori_loop(0, NG, columns, 0)
    local = lax.rem(lax.broadcasted_iota(jnp.int32, (128, 128), 0), OWN)

    def places(pp, carry):
        for h in range(2):
            at = slots[2 * pp + h][1:2, :].astype(jnp.int32)
            owner = at // OWN
            zrow[pp, :, h * 128 : (h + 1) * 128] = jnp.broadcast_to(
                jnp.where(owner % NX == x, (owner // NX).astype(F32), -1.0), (8, 128)
            )
            hit = jnp.broadcast_to(at % OWN, (128, 128)) == local
            bt[pp, :, h * 128 : (h + 1) * 128] = jnp.where(hit, 1.0, 0.0).astype(BF16)
        return carry

    acc[...] = jnp.zeros_like(acc)
    blank = jnp.zeros((16, 128 - FEAT), BF16)

    def operand(offs):
        sides = []
        for off in offs:
            cz = at_z(off)
            for d in (1, 3, 2):
                got(cz * NX + lax.rem(x + d, NX))
            blocks = [cg[cz * NX + b] for b in range(NX)]
            tails = [
                jnp.concatenate(
                    [one[16 * k : 16 * (k + 1), FEAT:] for k in range(3)] + [blank], axis=1
                )
                for one in blocks
            ]
            sides.append(jnp.concatenate(blocks + tails, axis=0))
        return jnp.concatenate(sides, axis=1)

    def choose(part, offs, hi, before):
        za, zb = (at_z(off).astype(F32) for off in offs)
        return jnp.where(hi == za, part[:, :128], jnp.where(hi == zb, part[:, 128:], before))

    def pick(offs):
        part = jnp.dot(low_hot[...], operand(offs), preferred_element_type=F32)
        acc[...] = choose(part, offs, high[...], acc[...])

    order = [0, 1, -1, 2, -2, 3, -3, 4, -4] + FAR
    pick(order[0:2])
    pick(order[2:4])
    for off in FAR[:4]:
        got(at_z(off) * NX + x)
        spread(off)
    pick(order[4:6])
    for off in FAR[4:]:
        got(at_z(off) * NX + x)
        spread(off)
    pick(order[6:8])
    for d in range(1, NG):
        book_got(d)
    lax.fori_loop(0, NG // 4, build_book, 0)
    for k in range(NZ // 2, NZ - 2, 2):
        pick(order[k : k + 2])

    def pick_copy(to, k):
        return pltpu.make_async_remote_copy(
            src_ref=wout.at[to], dst_ref=win.at[g],
            send_sem=ws_sem.at[k], recv_sem=w_sem.at[g],
            device_id=(gx, to), device_id_type=MESH,
        )

    last = order[NZ - 2 :]
    final = operand(last)
    y_me, core = g // 2, g % 2
    for dy in (2, 1, 3, 0):
        chip = lax.rem(y_me + dy, NG // 2)
        at = pl.ds(pl.multiple_of(chip * 2 * ROWS, 2 * ROWS), 2 * ROWS)
        part = jnp.dot(low_hot[at, :], final, preferred_element_type=F32)
        rows = choose(part, last, high[at, :], acc[at, :]).astype(BF16)
        for c in range(2):
            mine = rows[c * ROWS : (c + 1) * ROWS]
            for k in range(3):
                wout[2 * chip + c, 32 * k : 32 * (k + 1), :] = jnp.concatenate(
                    [mine[32 * k : 32 * (k + 1), :FEAT], mine[FEAT:, 32 * k : 32 * (k + 1)]], axis=1
                )
        if dy:
            for c in range(2):
                pick_copy(2 * chip + c, 2 * dy + c).start()
        else:
            pick_copy(2 * chip + 1 - core, 0).start()
    win[g] = wout[g]

    lax.fori_loop(NG // 4, NG // 2, build_book, 0)
    come = [g, 2 * y_me + 1 - core]
    for dy in (1, 3, 2):
        come += [2 * lax.rem(y_me + dy, NG // 2) + c for c in range(2)]
    for k, other in enumerate(come):
        if k:
            pltpu.make_async_remote_copy(
                src_ref=wout.at[0], dst_ref=win.at[other],
                send_sem=ws_sem.at[0], recv_sem=w_sem.at[other],
                device_id=(gx, g), device_id_type=MESH,
            ).wait_recv()
        packed = win[other]
        tail = jnp.concatenate([packed[32 * k : 32 * (k + 1), FEAT:] for k in range(3)], axis=1)
        rows = jnp.concatenate([packed[:, :FEAT], tail], axis=0)
        vr[...] += jnp.dot(
            rows, rot[pl.ds(pl.multiple_of(other * FEAT, 32), FEAT), :], preferred_element_type=F32
        )
    tt[...] = vr[...].T
    for j in range(NG):
        q, h = j // 2, j % 2
        part = tt[j * FEAT : (j + 1) * FEAT, :]
        wt[q, h * 128 : h * 128 + FEAT, h * 128 : (h + 1) * 128] = part.astype(BF16)
        qt[j * SUB : (j + 1) * SUB, :] = jnp.sum((part * part).reshape(SUB, 8, ROWS), axis=1)

    for q in range(NG // 2):
        for i in range(0, SUB, WIDE):
            dist = jnp.dot(
                book[q, i * CODES : (i + WIDE) * CODES, :], wt[q], preferred_element_type=F32
            )
            low = jnp.min(dist.reshape(WIDE, CODES, 256), axis=1)
            qmin[2 * q, i : i + WIDE, :] = low[:, :128]
            qmin[2 * q + 1, i : i + WIDE, :] = low[:, 128:]

    for j in range(NG):
        err = qt[j * SUB : (j + 1) * SUB, :] + qmin[j, 0:SUB, :]
        qt[j * SUB : (j + 1) * SUB, :] = err
        eout[j] = jnp.concatenate([err, jnp.ones((4, ROWS), F32)], axis=0).astype(BF16)

    def err_copy(dx, dg):
        return pltpu.make_async_remote_copy(
            src_ref=eout.at[g_to[dg]], dst_ref=ein.at[p_me],
            send_sem=es_sem.at[dx * NG + dg], recv_sem=e_sem.at[p_me],
            device_id=(gx_to[dx], g_to[dg]), device_id_type=MESH,
        )

    for dx, dg in plane:
        err_copy(dx, dg).start()
    ein[p_me] = eout[g]

    q_store = pltpu.make_async_copy(qt, q_hbm, out_sem.at[0])
    q_store.start()

    def err_got(other):
        pltpu.make_async_remote_copy(
            src_ref=eout.at[0], dst_ref=ein.at[other],
            send_sem=es_sem.at[0], recv_sem=e_sem.at[other],
            device_id=(gx, g), device_id_type=MESH,
        ).wait_recv()

    lax.fori_loop(0, NP // 2, places, 0)
    total = jnp.zeros((NZ * 16, 128), F32)
    for dx, dy in sorted(itertools.product(range(4), range(4)), key=lambda s: min(s[0], 4 - s[0]) + min(s[1], 4 - s[1])):
        pp = lax.rem(x + dx, 4) * 4 + lax.rem(y_me + dy, 4)
        if dx or dy:
            err_got(2 * pp)
            err_got(2 * pp + 1)
        else:
            err_got(2 * pp + 1 - core)
        for h in range(2):
            err = ein[2 * pp + h].astype(F32)
            owner = zrow[pp, 0:1, h * 128 : (h + 1) * 128]
            for a in range(NZ):
                lm[pp, a * 16 : (a + 1) * 16, h * 128 : (h + 1) * 128] = jnp.where(
                    owner == float(a), err, 0.0
                ).astype(BF16)
        total = total + lax.dot_general(
            lm[pp], bt[pp], (((1,), (1,)), ((), ())), preferred_element_type=F32
        )
    lane8 = lax.broadcasted_iota(jnp.int32, (8, 128), 1)
    for a in range(NZ):
        pout[a] = jnp.where(
            lane8 < OWN, total[a * 16 : a * 16 + 8, :], total[a * 16 + 8 : a * 16 + 16, :]
        ).astype(BF16)

    def sum_copy(d):
        to = at_z(d)
        return pltpu.make_async_remote_copy(
            src_ref=pout.at[to], dst_ref=pin.at[z],
            send_sem=ps_sem.at[d], recv_sem=p_sem.at[z],
            device_id=(to * NX + x, g), device_id_type=MESH,
        )

    for d in range(1, NZ):
        sum_copy(d).start()
    pin[z] = pout[z]
    for d in range(1, NZ):
        other = at_z(d)
        pltpu.make_async_remote_copy(
            src_ref=pout.at[0], dst_ref=pin.at[other],
            send_sem=ps_sem.at[0], recv_sem=p_sem.at[other],
            device_id=(gx, g), device_id_type=MESH,
        ).wait_recv()
    whole = jnp.sum(pin[...].astype(F32), axis=0)
    count = jnp.broadcast_to(whole[4:5, :], (8, 128))
    count = jnp.where(lane8 < OWN, pltpu.roll(count, OWN, 1), count)
    mean = whole / jnp.maximum(count, 1.0)
    lout[0:8, :] = mean[:, :OWN]
    lout[8:SUB, :] = pltpu.roll(mean, OWN, 1)[: SUB - 8, :OWN]
    l_store = pltpu.make_async_copy(lout, le_hbm, out_sem.at[1])
    l_store.start()

    for one in sent:
        one.wait_send()

    def x_done(bz, carry):
        for d in range(1, NX):
            x_copy(bz, d).wait_send()
        return carry

    lax.fori_loop(0, NZ, x_done, 0)
    for d in range(1, NG):
        book_copy(d).wait_send()
    for k in (0, 2, 3, 4, 5, 6, 7):
        pick_copy(0, k).wait_send()
    for dx, dg in plane:
        slot_copy(dx, dg).wait_send()
        err_copy(dx, dg).wait_send()

    for d in range(1, NZ):
        sum_copy(d).wait_send()
    q_store.wait()
    l_store.wait()


def on_device(vectors, list_ids, old_order, new_order, centroids, rotation, codebook):
    dma = pltpu.SemaphoreType.DMA
    any_spec = pl.BlockSpec(memory_space=pltpu.HBM)
    errors, means = pl.pallas_call(
        kernel,
        out_shape=(
            jax.ShapeDtypeStruct((NG * SUB, ROWS), F32),
            jax.ShapeDtypeStruct((SUB, OWN), F32),
        ),
        in_specs=[any_spec] * 7,
        out_specs=(any_spec, any_spec),
        scratch_shapes=[
            pltpu.VMEM((ROWS, 768), BF16),
            pltpu.VMEM((1, 128), jnp.int32),
            pltpu.VMEM((32, 128), jnp.int32),
            pltpu.VMEM((32, 128), jnp.int32),
            pltpu.VMEM((OWN, FEAT), BF16),
            pltpu.VMEM((NZ * NX, PACKED, 128), BF16),
            pltpu.VMEM((768, 768), BF16),
            pltpu.VMEM((NG, SUB, 8, CODES), BF16),
            pltpu.VMEM((2, 128), F32),
            pltpu.VMEM((NP, 2, 128), F32),
            pltpu.VMEM((NG * ROWS, 128), F32),
            pltpu.VMEM((NG * ROWS, 256), BF16),
            pltpu.VMEM((128, CODES), F32),
            pltpu.VMEM((NG // 2, SUB * CODES, 256), BF16),
            pltpu.VMEM((NG // 2, 256, 256), BF16),
            pltpu.VMEM((NG * ROWS, 128), F32),
            pltpu.VMEM((NG, FEAT, 128), BF16),
            pltpu.VMEM((NG, FEAT, 128), BF16),
            pltpu.VMEM((ROWS, 768), F32),
            pltpu.VMEM((NG, 16, ROWS), F32),
            pltpu.VMEM((768, ROWS), F32),
            pltpu.VMEM((NG * SUB, ROWS), F32),
            pltpu.VMEM((NG, 16, ROWS), BF16),
            pltpu.VMEM((NP, 16, ROWS), BF16),
            pltpu.VMEM((NP // 2, 8, 256), F32),
            pltpu.VMEM((NP // 2, 128, 256), BF16),
            pltpu.VMEM((NP // 2, NZ * 16, 256), BF16),
            pltpu.VMEM((NZ, 8, 128), BF16),
            pltpu.VMEM((NZ, 8, 128), BF16),
            pltpu.VMEM((SUB, OWN), F32),
            dma((7,)),
            dma((NZ,)),
            dma((NZ * NX,)),
            dma((NZ * NX,)),
            dma((NG,)),
            dma((NG,)),
            dma((NP,)),
            dma((NP,)),
            dma((NG,)),
            dma((NG,)),
            dma((NP,)),
            dma((NP,)),
            dma((NZ,)),
            dma((NZ,)),
            dma((2,)),
        ],
        compiler_params=pltpu.CompilerParams(
            collective_id=0, has_side_effects=True, vmem_limit_bytes=48 * 1024 * 1024
        ),
    )(
        *(
            pltpu.with_memory_space_constraint(one, pltpu.HBM)
            for one in (
                vectors,
                list_ids.reshape(1, ROWS),
                old_order.reshape(32, 128),
                new_order.reshape(32, 128),
                centroids,
                rotation,
                codebook,
            )
        )
    )
    return errors.T, means.T


def solution(mesh):
    both = ("gx", "gy")
    in_specs = (P(both, None), P(both), P(), P(), P("gx", "gy"), P(), P("gy", None, None))
    out_specs = (P(both, None), P("gx", "gy"))
    return jax.shard_map(
        on_device, mesh=mesh, in_specs=in_specs, out_specs=out_specs, check_vma=False
    )
```

```python
import jax
import jax.numpy as jnp
from jax import lax
from jax.experimental import pallas as pl
from jax.experimental.pallas import tpu as pltpu
from jax.sharding import PartitionSpec as P

MESH = pl.DeviceIdType.MESH
F32 = jnp.float32
BF16 = jnp.bfloat16

NZ, NX, NG = 16, 4, 8
NP = NX * NG
OWN = 64
FEAT = 96
SUB = 12
ROWS = 128
CODES = 256
CHUNK = 256
PACKED = OWN * FEAT // 128
WIDE = 6
HOP = 4
NEAR = [4, -4, 1, -1, 2, -2, 3, -3]
ARRIVAL = [
    (0, 0), (0, 2), (0, 3), (1, 2), (3, 2), (1, 3), (3, 3), (0, 1),
    (2, 2), (2, 3), (1, 1), (3, 1), (1, 0), (3, 0), (2, 1), (2, 0),
]
FAR = [5, -5, 6, -6, 7, -7, 8]


def kernel(
    v_hbm, ids_hbm, old_hbm, new_hbm, c_hbm, r_hbm, cb_hbm,
    q_ref, mean_ref,
    v, ids, old, new, block_in, cg, rot, cb,
    slot_out, slots, high, low_hot, y, book, wt, acc, wout, win, vr,
    qmin, tt, eout, ein, zrow, bt, lm, pout, pin,
    in_sem, zs_sem, xs_sem, ag_sem, cbs_sem, cb_sem, sls_sem, sl_sem,
    ws_sem, w_sem, es_sem, e_sem, ps_sem, p_sem,
):
    gx, g = lax.axis_index("gx"), lax.axis_index("gy")
    z, x = gx // NX, gx % NX
    p_me = x * NG + g

    def at_z(off):
        return lax.rem(z + (off + NZ), NZ)

    x_to = [lax.rem(x + d, NX) for d in range(NX)]
    g_to = [lax.rem(g + d, NG) for d in range(NG)]
    gx_to = [z * NX + one for one in x_to]
    plane = [(dx, dg) for dx in (2, 1, 3, 0) for dg in (4, 5, 2, 3, 6, 7, 1, 0) if dx or dg]

    barrier = pltpu.get_barrier_semaphore()
    for off in NEAR:
        pl.semaphore_signal(barrier, inc=1, device_id=(at_z(off) * NX + x, g), device_id_type=MESH)

    for dx, dg in plane:
        pl.semaphore_signal(barrier, inc=1, device_id=(gx_to[dx], g_to[dg]), device_id_type=MESH)

    loads = [
        pltpu.make_async_copy(c_hbm, block_in, in_sem.at[0]),
        pltpu.make_async_copy(ids_hbm, ids, in_sem.at[1]),
        pltpu.make_async_copy(old_hbm, old, in_sem.at[2]),
        pltpu.make_async_copy(new_hbm, new, in_sem.at[3]),
        pltpu.make_async_copy(cb_hbm, cb.at[g], in_sem.at[4]),
        pltpu.make_async_copy(v_hbm, v, in_sem.at[5]),
        pltpu.make_async_copy(r_hbm, rot, in_sem.at[6]),
    ]
    for one in loads:
        one.start()

    loads[0].wait()
    for k in range(3):
        tail = block_in[48:64, 32 * k : 32 * (k + 1)]
        cg[gx, 16 * k : 16 * (k + 1), :] = jnp.concatenate(
            [block_in[16 * k : 16 * (k + 1), :], tail], axis=1
        )
    pl.semaphore_wait(barrier, len(NEAR) + NP - 1)

    def z_copy(block_z, to_off, k):
        block = block_z * NX + x
        return pltpu.make_async_remote_copy(
            src_ref=cg.at[block], dst_ref=cg.at[block],
            send_sem=zs_sem.at[k], recv_sem=ag_sem.at[block],
            device_id=(at_z(to_off) * NX + x, g), device_id_type=MESH,
        )

    def x_copy(block_z, d):
        block = block_z * NX + x
        return pltpu.make_async_remote_copy(
            src_ref=cg.at[block], dst_ref=cg.at[block],
            send_sem=xs_sem.at[block_z * NX + d], recv_sem=ag_sem.at[block],
            device_id=(z * NX + lax.rem(x + d, NX), g), device_id_type=MESH,
        )

    def got(block):
        pltpu.make_async_remote_copy(
            src_ref=cg.at[block], dst_ref=cg.at[block],
            send_sem=zs_sem.at[0], recv_sem=ag_sem.at[block],
            device_id=(gx, g), device_id_type=MESH,
        ).wait_recv()

    sent = []
    for k, off in enumerate(NEAR):
        sent.append(z_copy(z, off, k))
        sent[-1].start()
    for d in (1, 3, 2):
        x_copy(z, d).start()

    for k in (1, 2, 3):
        loads[k].wait()
    lane = lax.broadcasted_iota(jnp.int32, (ROWS, 128), 1)
    lane_f = lane.astype(F32)
    id_col = jnp.broadcast_to(ids[...].astype(F32), (ROWS, 128)).T

    def find(order, row):
        total = jnp.zeros((ROWS, 128), F32)
        for k in range(32):
            entry = jnp.broadcast_to(order[k : k + 1, :].astype(F32), (ROWS, 128))
            total = total + jnp.where(id_col == entry, lane_f + float(128 * k), 0.0)
        slot_out[row : row + 1, :] = jnp.sum(total.T, axis=0, keepdims=True)

    find(old, 0)
    find(new, 1)

    def slot_copy(dx, dg):
        return pltpu.make_async_remote_copy(
            src_ref=slot_out, dst_ref=slots.at[p_me],
            send_sem=sls_sem.at[dx * NG + dg], recv_sem=sl_sem.at[p_me],
            device_id=(gx_to[dx], g_to[dg]), device_id_type=MESH,
        )

    for dx, dg in plane:
        slot_copy(dx, dg).start()
    slots[p_me] = slot_out[...]

    def book_copy(d):
        return pltpu.make_async_remote_copy(
            src_ref=cb.at[g], dst_ref=cb.at[g],
            send_sem=cbs_sem.at[d], recv_sem=cb_sem.at[g],
            device_id=(gx, lax.rem(g + d, NG)), device_id_type=MESH,
        )

    loads[4].wait()
    for d in range(1, NG):
        book_copy(d).start()

    loads[5].wait()
    loads[6].wait()
    vr[...] = jnp.dot(v[...], rot[...], preferred_element_type=F32)

    def spread(off):
        for d in (2, 1, 3):
            x_copy(at_z(off), d).start()

    for off in NEAR[2:6]:
        got(at_z(off) * NX + x)
        spread(off)
    k = len(NEAR)
    for off in NEAR[:2]:
        got(at_z(off) * NX + x)
        step = -1 if off > 0 else 1
        for far in range(HOP if off > 0 else HOP - 1, 0, -1):
            sent.append(z_copy(at_z(off), step * far, k))
            sent[-1].start()
            k += 1
    for off in NEAR[6:] + NEAR[:2]:
        if abs(off) < HOP:
            got(at_z(off) * NX + x)
        spread(off)

    y[...] = jnp.zeros_like(y)
    wt[...] = jnp.zeros_like(wt)
    for q in range(NG // 2):
        for h in range(2):
            wt[q, h * 128 + FEAT : (h + 1) * 128, h * 128 : (h + 1) * 128] = jnp.ones((32, 128), BF16)

    def book_got(d):
        other = lax.rem(g + d, NG)
        pltpu.make_async_remote_copy(
            src_ref=cb.at[other], dst_ref=cb.at[other],
            send_sem=cbs_sem.at[0], recv_sem=cb_sem.at[other],
            device_id=(gx, g), device_id_type=MESH,
        ).wait_recv()

    lane_row = lax.broadcasted_iota(jnp.int32, (1, 128), 1)
    member = jnp.where(lane_row < FEAT, lane_row // 8, lax.rem(lane_row - FEAT, 16))

    def build_book(q, carry):
        for h in range(2):
            words = cb[2 * q + h].astype(F32)
            norm = jnp.sum(words * words, axis=1)
            high = norm.astype(BF16).astype(F32)
            y[0:FEAT, :] = -2.0 * words.reshape(FEAT, CODES)
            y[FEAT : FEAT + SUB, :] = high
            y[FEAT + 16 : FEAT + 16 + SUB, :] = (norm - high).astype(BF16).astype(F32)
            turned_words = y[...].T.astype(BF16)
            for i in range(SUB):
                mask = jnp.where(member == i, 1.0, 0.0).astype(BF16)
                book[q, i * CODES : (i + 1) * CODES, h * 128 : (h + 1) * 128] = turned_words * mask
        return carry


    def slot_got(d, carry):
        other = lax.rem(p_me + d, NP)
        pltpu.make_async_remote_copy(
            src_ref=slot_out, dst_ref=slots.at[other],
            send_sem=sls_sem.at[0], recv_sem=sl_sem.at[other],
            device_id=(gx, g), device_id_type=MESH,
        ).wait_recv()
        return carry

    lax.fori_loop(1, NP, slot_got, 0)

    def columns(j, carry):
        row = slots[x * NG + j][0:1, :].astype(jnp.int32)
        at = pl.ds(pl.multiple_of(j * ROWS, ROWS), ROWS)
        high[at, :] = jnp.broadcast_to((row // CHUNK).astype(F32), (ROWS, 128)).T
        inner = row % CHUNK
        block, spot = inner // OWN, inner % OWN
        place = jnp.where(spot < 48, block * 48 + spot, 144 + block * 16 + spot)
        rest = jnp.broadcast_to(place.astype(F32), (ROWS, 128)).T
        for h in range(2):
            low_hot[at, h * 128 : (h + 1) * 128] = jnp.where(
                rest == lane_f + float(128 * h), -1.0, 0.0
            ).astype(BF16)
        return carry

    lax.fori_loop(0, NG, columns, 0)
    local = lax.rem(lax.broadcasted_iota(jnp.int32, (128, 128), 0), OWN)

    def places(pp, carry):
        for h in range(2):
            at = slots[2 * pp + h][1:2, :].astype(jnp.int32)
            owner = at // OWN
            zrow[pp, :, h * 128 : (h + 1) * 128] = jnp.broadcast_to(
                jnp.where(owner % NX == x, (owner // NX).astype(F32), -1.0), (8, 128)
            )
            hit = jnp.broadcast_to(at % OWN, (128, 128)) == local
            bt[pp, :, h * 128 : (h + 1) * 128] = jnp.where(hit, 1.0, 0.0).astype(BF16)
        return carry

    acc[...] = jnp.zeros_like(acc)
    blank = jnp.zeros((16, 128 - FEAT), BF16)

    def operand(offs):
        sides = []
        for off in offs:
            cz = at_z(off)
            for d in (1, 3, 2):
                got(cz * NX + lax.rem(x + d, NX))
            blocks = [cg[cz * NX + b] for b in range(NX)]
            tails = [
                jnp.concatenate(
                    [one[16 * k : 16 * (k + 1), FEAT:] for k in range(3)] + [blank], axis=1
                )
                for one in blocks
            ]
            sides.append(jnp.concatenate(blocks + tails, axis=0))
        return jnp.concatenate(sides, axis=1)

    def choose(part, offs, hi, before):
        za, zb = (at_z(off).astype(F32) for off in offs)
        return jnp.where(hi == za, part[:, :128], jnp.where(hi == zb, part[:, 128:], before))

    def pick(offs):
        part = jnp.dot(low_hot[...], operand(offs), preferred_element_type=F32)
        acc[...] = choose(part, offs, high[...], acc[...])

    order = [0, 1, -1, 2, -2, 3, -3, 4, -4] + FAR

    def pass_on(offs):
        for off in offs:
            got(at_z(off) * NX + x)
            spread(off)

    pick(order[0:2])
    pass_on(FAR[0:2])
    pick(order[2:4])
    pass_on(FAR[2:4])
    pick(order[4:6])
    pass_on(FAR[4:])
    pick(order[6:8])
    for d in range(1, NG):
        book_got(d)
    lax.fori_loop(0, NG // 4, build_book, 0)
    for k in range(NZ // 2, NZ - 2, 2):
        pick(order[k : k + 2])

    def pick_copy(to, k):
        return pltpu.make_async_remote_copy(
            src_ref=wout.at[to], dst_ref=win.at[g],
            send_sem=ws_sem.at[k], recv_sem=w_sem.at[g],
            device_id=(gx, to), device_id_type=MESH,
        )

    last = order[NZ - 2 :]
    final = operand(last)
    y_me, core = g // 2, g % 2
    for dy in (2, 1, 3, 0):
        chip = lax.rem(y_me + dy, NG // 2)
        at = pl.ds(pl.multiple_of(chip * 2 * ROWS, 2 * ROWS), 2 * ROWS)
        part = jnp.dot(low_hot[at, :], final, preferred_element_type=F32)
        rows = choose(part, last, high[at, :], acc[at, :]).astype(BF16)
        for c in range(2):
            mine = rows[c * ROWS : (c + 1) * ROWS]
            for k in range(3):
                wout[2 * chip + c, 32 * k : 32 * (k + 1), :] = jnp.concatenate(
                    [mine[32 * k : 32 * (k + 1), :FEAT], mine[FEAT:, 32 * k : 32 * (k + 1)]], axis=1
                )
        if dy:
            for c in range(2):
                pick_copy(2 * chip + c, 2 * dy + c).start()
        else:
            pick_copy(2 * chip + 1 - core, 0).start()
    win[g] = wout[g]

    lax.fori_loop(NG // 4, NG // 2, build_book, 0)
    chips = [[2 * lax.rem(y_me + dy, NG // 2) + c for c in range(2)] for dy in (1, 3, 2)]
    for group in ([g, 2 * y_me + 1 - core], chips[0], chips[1] + chips[2]):
        for other in group:
            if other is not g:
                pltpu.make_async_remote_copy(
                    src_ref=wout.at[0], dst_ref=win.at[other],
                    send_sem=ws_sem.at[0], recv_sem=w_sem.at[other],
                    device_id=(gx, g), device_id_type=MESH,
                ).wait_recv()
        moved = None
        for other in group:
            packed = win[other]
            tail = jnp.concatenate([packed[32 * k : 32 * (k + 1), FEAT:] for k in range(3)], axis=1)
            rows = jnp.concatenate([packed[:, :FEAT], tail], axis=0)
            part = jnp.dot(
                rows, rot[pl.ds(pl.multiple_of(other * FEAT, 32), FEAT), :], preferred_element_type=F32
            )
            moved = part if moved is None else moved + part
        vr[...] += moved
    tt[...] = vr[...].T
    for j in range(NG):
        q, h = j // 2, j % 2
        part = tt[j * FEAT : (j + 1) * FEAT, :]
        wt[q, h * 128 : h * 128 + FEAT, h * 128 : (h + 1) * 128] = part.astype(BF16)
        qmin[j, 0:SUB, :] = jnp.sum((part * part).reshape(SUB, 8, ROWS), axis=1)

    def err_copy(dx, to, k):
        return pltpu.make_async_remote_copy(
            src_ref=eout.at[to], dst_ref=ein.at[p_me],
            send_sem=es_sem.at[k], recv_sem=e_sem.at[p_me],
            device_id=(gx_to[dx], to), device_id_type=MESH,
        )

    spare = jnp.ones((4, ROWS), F32)
    err_sent = []
    for dy in (2, 1, 3, 0):
        q = lax.rem(y_me + dy, NG // 2)
        for i in range(0, SUB, WIDE):
            dist = jnp.dot(
                book[q, i * CODES : (i + WIDE) * CODES, :], wt[q], preferred_element_type=F32
            )
            low = jnp.min(dist.reshape(WIDE, CODES, 256), axis=1)
            qmin[2 * q, i : i + WIDE, :] += low[:, :128]
            qmin[2 * q + 1, i : i + WIDE, :] += low[:, 128:]
        for c in range(2):
            eout[2 * q + c] = jnp.concatenate([qmin[2 * q + c, 0:SUB, :], spare], axis=0).astype(BF16)
        for dx in (2, 1, 3, 0):
            for c in range(2) if dx or dy else (0,):
                to = 2 * q + c if dx or dy else 2 * q + 1 - core
                err_sent.append(err_copy(dx, to, len(err_sent)))
                err_sent[-1].start()
    ein[p_me] = eout[g]

    for j in range(NG):
        q_ref[j * SUB : (j + 1) * SUB, :] = qmin[j, 0:SUB, :]

    def err_got(other):
        pltpu.make_async_remote_copy(
            src_ref=eout.at[0], dst_ref=ein.at[other],
            send_sem=es_sem.at[0], recv_sem=e_sem.at[other],
            device_id=(gx, g), device_id_type=MESH,
        ).wait_recv()

    lax.fori_loop(0, NP // 2, places, 0)
    total = jnp.zeros((NZ * 16, 128), F32)
    for dx, dy in ARRIVAL:
        pp = lax.rem(x + dx, 4) * 4 + lax.rem(y_me + dy, 4)
        if dx or dy:
            err_got(2 * pp)
            err_got(2 * pp + 1)
        else:
            err_got(2 * pp + 1 - core)
        for h in range(2):
            err = ein[2 * pp + h].astype(F32)
            owner = zrow[pp, 0:1, h * 128 : (h + 1) * 128]
            for a in range(NZ):
                lm[pp, a * 16 : (a + 1) * 16, h * 128 : (h + 1) * 128] = jnp.where(
                    owner == float(a), err, 0.0
                ).astype(BF16)
        total = total + lax.dot_general(
            lm[pp], bt[pp], (((1,), (1,)), ((), ())), preferred_element_type=F32
        )
    lane8 = lax.broadcasted_iota(jnp.int32, (8, 128), 1)
    for a in range(NZ):
        pout[a] = jnp.where(
            lane8 < OWN, total[a * 16 : a * 16 + 8, :], total[a * 16 + 8 : a * 16 + 16, :]
        ).astype(BF16)

    def sum_copy(d):
        to = at_z(d)
        return pltpu.make_async_remote_copy(
            src_ref=pout.at[to], dst_ref=pin.at[z],
            send_sem=ps_sem.at[d], recv_sem=p_sem.at[z],
            device_id=(to * NX + x, g), device_id_type=MESH,
        )

    for d in (8, 7, 9, 6, 10, 5, 11, 4, 12, 3, 13, 2, 14, 1, 15):
        sum_copy(d).start()
    pin[z] = pout[z]
    for one in sent + err_sent:
        one.wait_send()

    def x_done(bz, carry):
        for d in range(1, NX):
            x_copy(bz, d).wait_send()
        return carry

    lax.fori_loop(0, NZ, x_done, 0)
    for d in range(1, NG):
        book_copy(d).wait_send()
    for k in (0, 2, 3, 4, 5, 6, 7):
        pick_copy(0, k).wait_send()
    for dx, dg in plane:
        slot_copy(dx, dg).wait_send()

    for d in range(1, NZ):
        other = at_z(d)
        pltpu.make_async_remote_copy(
            src_ref=pout.at[0], dst_ref=pin.at[other],
            send_sem=ps_sem.at[0], recv_sem=p_sem.at[other],
            device_id=(gx, g), device_id_type=MESH,
        ).wait_recv()
    whole = jnp.sum(pin[...].astype(F32), axis=0)
    count = jnp.broadcast_to(whole[4:5, :], (8, 128))
    count = jnp.where(lane8 < OWN, pltpu.roll(count, OWN, 1), count)
    mean = whole / jnp.maximum(count, 1.0)
    mean_ref[0:8, :] = mean[:, :OWN]
    mean_ref[8:SUB, :] = pltpu.roll(mean, OWN, 1)[: SUB - 8, :OWN]

    for d in range(1, NZ):
        sum_copy(d).wait_send()


def on_device(vectors, list_ids, old_order, new_order, centroids, rotation, codebook):
    dma = pltpu.SemaphoreType.DMA
    any_spec = pl.BlockSpec(memory_space=pltpu.HBM)
    errors, means = pl.pallas_call(
        kernel,
        out_shape=(
            jax.ShapeDtypeStruct((NG * SUB, ROWS), F32),
            jax.ShapeDtypeStruct((SUB, OWN), F32),
        ),
        in_specs=[any_spec] * 7,
        out_specs=(pl.BlockSpec(memory_space=pltpu.VMEM),) * 2,
        scratch_shapes=[
            pltpu.VMEM((ROWS, 768), BF16),
            pltpu.VMEM((1, 128), jnp.int32),
            pltpu.VMEM((32, 128), jnp.int32),
            pltpu.VMEM((32, 128), jnp.int32),
            pltpu.VMEM((OWN, FEAT), BF16),
            pltpu.VMEM((NZ * NX, PACKED, 128), BF16),
            pltpu.VMEM((768, 768), BF16),
            pltpu.VMEM((NG, SUB, 8, CODES), BF16),
            pltpu.VMEM((2, 128), F32),
            pltpu.VMEM((NP, 2, 128), F32),
            pltpu.VMEM((NG * ROWS, 128), F32),
            pltpu.VMEM((NG * ROWS, 256), BF16),
            pltpu.VMEM((128, CODES), F32),
            pltpu.VMEM((NG // 2, SUB * CODES, 256), BF16),
            pltpu.VMEM((NG // 2, 256, 256), BF16),
            pltpu.VMEM((NG * ROWS, 128), F32),
            pltpu.VMEM((NG, FEAT, 128), BF16),
            pltpu.VMEM((NG, FEAT, 128), BF16),
            pltpu.VMEM((ROWS, 768), F32),
            pltpu.VMEM((NG, 16, ROWS), F32),
            pltpu.VMEM((768, ROWS), F32),
            pltpu.VMEM((NG, 16, ROWS), BF16),
            pltpu.VMEM((NP, 16, ROWS), BF16),
            pltpu.VMEM((NP // 2, 8, 256), F32),
            pltpu.VMEM((NP // 2, 128, 256), BF16),
            pltpu.VMEM((NP // 2, NZ * 16, 256), BF16),
            pltpu.VMEM((NZ, 8, 128), BF16),
            pltpu.VMEM((NZ, 8, 128), BF16),
            dma((7,)),
            dma((NZ,)),
            dma((NZ * NX,)),
            dma((NZ * NX,)),
            dma((NG,)),
            dma((NG,)),
            dma((NP,)),
            dma((NP,)),
            dma((NG,)),
            dma((NG,)),
            dma((NP,)),
            dma((NP,)),
            dma((NZ,)),
            dma((NZ,)),
        ],
        compiler_params=pltpu.CompilerParams(
            collective_id=0, has_side_effects=True, vmem_limit_bytes=48 * 1024 * 1024
        ),
    )(
        *(
            pltpu.with_memory_space_constraint(one, pltpu.HBM)
            for one in (
                vectors,
                list_ids.reshape(1, ROWS),
                old_order.reshape(32, 128),
                new_order.reshape(32, 128),
                centroids,
                rotation,
                codebook,
            )
        )
    )
    return errors.T, means.T


def solution(mesh):
    both = ("gx", "gy")
    in_specs = (P(both, None), P(both), P(), P(), P("gx", "gy"), P(), P("gy", None, None))
    out_specs = (P(both, None), P("gx", "gy"))
    return jax.shard_map(
        on_device, mesh=mesh, in_specs=in_specs, out_specs=out_specs, check_vma=False
    )
```

```python
import jax
import jax.numpy as jnp
from jax import lax
from jax.experimental import pallas as pl
from jax.experimental.pallas import tpu as pltpu
from jax.sharding import PartitionSpec as P

MESH = pl.DeviceIdType.MESH
F32 = jnp.float32
BF16 = jnp.bfloat16

NZ, NX, NG = 16, 4, 8
NP = NX * NG
OWN = 64
FEAT = 96
SUB = 12
ROWS = 128
CODES = 256
CHUNK = 256
PACKED = OWN * FEAT // 128
WIDE = 6
HOP = 4
NEAR = [4, -4, 1, -1, 2, -2, 3, -3]
ARRIVAL = [
    (0, 0), (0, 2), (0, 3), (1, 2), (3, 2), (1, 3), (3, 3), (0, 1),
    (2, 2), (2, 3), (1, 1), (3, 1), (1, 0), (3, 0), (2, 1), (2, 0),
]
FAR = [5, -5, 6, -6, 7, -7, 8]
ORDER = [0, 1, -1, 2, -2, 3, -3, 4, -4] + FAR


def kernel(
    v_hbm, ids_hbm, old_hbm, new_hbm, c_hbm, r_hbm, cb_hbm,
    q_ref, mean_ref,
    v, ids, old, new, block_in, cg, rot, cb,
    slot_out, slots, high, low_hot, y, book, wt, acc, wout, win, vr,
    qmin, tt, eout, ein, zrow, bt, lm, pout, pin,
    in_sem, zs_sem, xs_sem, ag_sem, ax_sem, cbs_sem, cb_sem, sls_sem, sl_sem,
    ws_sem, w_sem, es_sem, e_sem, ps_sem, p_sem,
):
    gx, g = lax.axis_index("gx"), lax.axis_index("gy")
    z, x = gx // NX, gx % NX
    p_me = x * NG + g

    def at_z(off):
        return lax.rem(z + (off + NZ), NZ)

    x_to = [lax.rem(x + d, NX) for d in range(NX)]
    g_to = [lax.rem(g + d, NG) for d in range(NG)]
    gx_to = [z * NX + one for one in x_to]
    plane = [(dx, dg) for dx in (2, 1, 3, 0) for dg in (4, 5, 2, 3, 6, 7, 1, 0) if dx or dg]

    barrier = pltpu.get_barrier_semaphore()
    for off in NEAR:
        pl.semaphore_signal(barrier, inc=1, device_id=(at_z(off) * NX + x, g), device_id_type=MESH)

    for dx, dg in plane:
        pl.semaphore_signal(barrier, inc=1, device_id=(gx_to[dx], g_to[dg]), device_id_type=MESH)

    loads = [
        pltpu.make_async_copy(c_hbm, block_in, in_sem.at[0]),
        pltpu.make_async_copy(ids_hbm, ids, in_sem.at[1]),
        pltpu.make_async_copy(old_hbm, old, in_sem.at[2]),
        pltpu.make_async_copy(new_hbm, new, in_sem.at[3]),
        pltpu.make_async_copy(cb_hbm, cb.at[g], in_sem.at[4]),
        pltpu.make_async_copy(v_hbm, v, in_sem.at[5]),
        pltpu.make_async_copy(r_hbm, rot, in_sem.at[6]),
    ]
    for one in loads:
        one.start()

    loads[0].wait()
    for k in range(3):
        tail = block_in[48:64, 32 * k : 32 * (k + 1)]
        cg[gx, 16 * k : 16 * (k + 1), :] = jnp.concatenate(
            [block_in[16 * k : 16 * (k + 1), :], tail], axis=1
        )
    pl.semaphore_wait(barrier, len(NEAR) + NP - 1)

    def all_of(ref, sem):
        return pltpu.make_async_remote_copy(
            src_ref=ref, dst_ref=ref, send_sem=sem, recv_sem=sem,
            device_id=(gx, g), device_id_type=MESH,
        )

    def z_copy(block_z, to_off):
        block = block_z * NX + x
        return pltpu.make_async_remote_copy(
            src_ref=cg.at[block], dst_ref=cg.at[block],
            send_sem=zs_sem, recv_sem=ag_sem.at[block_z],
            device_id=(at_z(to_off) * NX + x, g), device_id_type=MESH,
        )

    def x_copy(off, d):
        block = at_z(off) * NX + x
        return pltpu.make_async_remote_copy(
            src_ref=cg.at[block], dst_ref=cg.at[block],
            send_sem=xs_sem, recv_sem=ax_sem.at[ORDER.index(off) // 2],
            device_id=(gx_to[d], g), device_id_type=MESH,
        )

    def got(off):
        all_of(cg.at[0], ag_sem.at[at_z(off)]).wait_recv()

    for off in NEAR:
        z_copy(z, off).start()
    for d in (1, 3, 2):
        x_copy(0, d).start()

    for k in (1, 2, 3):
        loads[k].wait()
    lane = lax.broadcasted_iota(jnp.int32, (ROWS, 128), 1)
    lane_f = lane.astype(F32)
    id_col = jnp.broadcast_to(ids[...].astype(F32), (ROWS, 128)).T

    def find(order, row):
        total = jnp.zeros((ROWS, 128), F32)
        for k in range(32):
            entry = jnp.broadcast_to(order[k : k + 1, :].astype(F32), (ROWS, 128))
            total = total + jnp.where(id_col == entry, lane_f + float(128 * k), 0.0)
        slot_out[row : row + 1, :] = jnp.sum(total.T, axis=0, keepdims=True)

    find(old, 0)
    find(new, 1)

    def slot_copy(dx, dg):
        return pltpu.make_async_remote_copy(
            src_ref=slot_out, dst_ref=slots.at[p_me],
            send_sem=sls_sem, recv_sem=sl_sem,
            device_id=(gx_to[dx], g_to[dg]), device_id_type=MESH,
        )

    for dx, dg in plane:
        slot_copy(dx, dg).start()
    slots[p_me] = slot_out[...]

    def book_copy(d):
        return pltpu.make_async_remote_copy(
            src_ref=cb.at[g], dst_ref=cb.at[g],
            send_sem=cbs_sem, recv_sem=cb_sem,
            device_id=(gx, lax.rem(g + d, NG)), device_id_type=MESH,
        )

    loads[4].wait()
    for d in range(1, NG):
        book_copy(d).start()

    loads[5].wait()
    loads[6].wait()
    vr[...] = jnp.dot(v[...], rot[...], preferred_element_type=F32)

    def spread(off):
        for d in (2, 1, 3):
            x_copy(off, d).start()

    for off in NEAR[2:6]:
        got(off)
        spread(off)
    for off in NEAR[:2]:
        got(off)
        step = -1 if off > 0 else 1
        for far in range(HOP if off > 0 else HOP - 1, 0, -1):
            z_copy(at_z(off), step * far).start()
    for off in NEAR[6:] + NEAR[:2]:
        if abs(off) < HOP:
            got(off)
        spread(off)

    y[...] = jnp.zeros_like(y)
    wt[...] = jnp.zeros_like(wt)
    for q in range(NG // 2):
        for h in range(2):
            wt[q, h * 128 + FEAT : (h + 1) * 128, h * 128 : (h + 1) * 128] = jnp.ones((32, 128), BF16)

    lane_row = lax.broadcasted_iota(jnp.int32, (1, 128), 1)
    member = jnp.where(lane_row < FEAT, lane_row // 8, lax.rem(lane_row - FEAT, 16))

    def build_book(q, carry):
        for h in range(2):
            words = cb[2 * q + h].astype(F32)
            norm = jnp.sum(words * words, axis=1)
            high = norm.astype(BF16).astype(F32)
            y[0:FEAT, :] = -2.0 * words.reshape(FEAT, CODES)
            y[FEAT : FEAT + SUB, :] = high
            y[FEAT + 16 : FEAT + 16 + SUB, :] = (norm - high).astype(BF16).astype(F32)
            turned_words = y[...].T.astype(BF16)
            for i in range(SUB):
                mask = jnp.where(member == i, 1.0, 0.0).astype(BF16)
                book[q, i * CODES : (i + 1) * CODES, h * 128 : (h + 1) * 128] = turned_words * mask
        return carry


    all_of(slots.at[0 : NP - 1], sl_sem).wait_recv()

    def columns(j, carry):
        row = slots[x * NG + j][0:1, :].astype(jnp.int32)
        at = pl.ds(pl.multiple_of(j * ROWS, ROWS), ROWS)
        high[at, :] = jnp.broadcast_to((row // CHUNK).astype(F32), (ROWS, 128)).T
        inner = row % CHUNK
        block, spot = inner // OWN, inner % OWN
        place = jnp.where(spot < 48, block * 48 + spot, 144 + block * 16 + spot)
        rest = jnp.broadcast_to(place.astype(F32), (ROWS, 128)).T
        for h in range(2):
            low_hot[at, h * 128 : (h + 1) * 128] = jnp.where(
                rest == lane_f + float(128 * h), -1.0, 0.0
            ).astype(BF16)
        return carry

    lax.fori_loop(0, NG, columns, 0)
    local = lax.rem(lax.broadcasted_iota(jnp.int32, (128, 128), 0), OWN)

    def places(pp, carry):
        for h in range(2):
            at = slots[2 * pp + h][1:2, :].astype(jnp.int32)
            owner = at // OWN
            zrow[pp, :, h * 128 : (h + 1) * 128] = jnp.broadcast_to(
                jnp.where(owner % NX == x, (owner // NX).astype(F32), -1.0), (8, 128)
            )
            hit = jnp.broadcast_to(at % OWN, (128, 128)) == local
            bt[pp, :, h * 128 : (h + 1) * 128] = jnp.where(hit, 1.0, 0.0).astype(BF16)
        return carry

    acc[...] = jnp.zeros_like(acc)
    blank = jnp.zeros((16, 128 - FEAT), BF16)

    def operand(offs):
        all_of(cg.at[0:6], ax_sem.at[ORDER.index(offs[0]) // 2]).wait_recv()
        sides = []
        for off in offs:
            cz = at_z(off)
            blocks = [cg[cz * NX + b] for b in range(NX)]
            tails = [
                jnp.concatenate(
                    [one[16 * k : 16 * (k + 1), FEAT:] for k in range(3)] + [blank], axis=1
                )
                for one in blocks
            ]
            sides.append(jnp.concatenate(blocks + tails, axis=0))
        return jnp.concatenate(sides, axis=1)

    def choose(part, offs, hi, before):
        za, zb = (at_z(off).astype(F32) for off in offs)
        return jnp.where(hi == za, part[:, :128], jnp.where(hi == zb, part[:, 128:], before))

    def pick(offs):
        part = jnp.dot(low_hot[...], operand(offs), preferred_element_type=F32)
        acc[...] = choose(part, offs, high[...], acc[...])


    def pass_on(offs):
        for off in offs:
            got(off)
            spread(off)

    pick(ORDER[0:2])
    pass_on(FAR[0:2])
    pick(ORDER[2:4])
    pass_on(FAR[2:4])
    pick(ORDER[4:6])
    pass_on(FAR[4:])
    pick(ORDER[6:8])
    all_of(cb.at[0 : NG - 1], cb_sem).wait_recv()
    lax.fori_loop(0, NG // 4, build_book, 0)
    for k in range(NZ // 2, NZ - 2, 2):
        pick(ORDER[k : k + 2])

    def pick_copy(to):
        return pltpu.make_async_remote_copy(
            src_ref=wout.at[to], dst_ref=win.at[g],
            send_sem=ws_sem, recv_sem=w_sem.at[g // 2],
            device_id=(gx, to), device_id_type=MESH,
        )

    last = ORDER[NZ - 2 :]
    final = operand(last)
    y_me, core = g // 2, g % 2
    for dy in (2, 1, 3, 0):
        chip = lax.rem(y_me + dy, NG // 2)
        at = pl.ds(pl.multiple_of(chip * 2 * ROWS, 2 * ROWS), 2 * ROWS)
        part = jnp.dot(low_hot[at, :], final, preferred_element_type=F32)
        rows = choose(part, last, high[at, :], acc[at, :]).astype(BF16)
        for c in range(2):
            mine = rows[c * ROWS : (c + 1) * ROWS]
            for k in range(3):
                wout[2 * chip + c, 32 * k : 32 * (k + 1), :] = jnp.concatenate(
                    [mine[32 * k : 32 * (k + 1), :FEAT], mine[FEAT:, 32 * k : 32 * (k + 1)]], axis=1
                )
        if dy:
            for c in range(2):
                pick_copy(2 * chip + c).start()
        else:
            pick_copy(2 * chip + 1 - core).start()
    win[g] = wout[g]

    lax.fori_loop(NG // 4, NG // 2, build_book, 0)
    chips = [[2 * lax.rem(y_me + dy, NG // 2) + c for c in range(2)] for dy in (1, 3, 2)]
    for dys, group in (((0,), [g, 2 * y_me + 1 - core]), ((1,), chips[0]), ((3, 2), chips[1] + chips[2])):
        for dy in dys:
            all_of(win.at[0 : 2 if dy else 1], w_sem.at[lax.rem(y_me + dy, NG // 2)]).wait_recv()
        moved = None
        for other in group:
            packed = win[other]
            tail = jnp.concatenate([packed[32 * k : 32 * (k + 1), FEAT:] for k in range(3)], axis=1)
            rows = jnp.concatenate([packed[:, :FEAT], tail], axis=0)
            part = jnp.dot(
                rows, rot[pl.ds(pl.multiple_of(other * FEAT, 32), FEAT), :], preferred_element_type=F32
            )
            moved = part if moved is None else moved + part
        vr[...] += moved
    tt[...] = vr[...].T
    for j in range(NG):
        q, h = j // 2, j % 2
        part = tt[j * FEAT : (j + 1) * FEAT, :]
        wt[q, h * 128 : h * 128 + FEAT, h * 128 : (h + 1) * 128] = part.astype(BF16)
        qmin[j, 0:SUB, :] = jnp.sum((part * part).reshape(SUB, 8, ROWS), axis=1)

    def err_copy(dx, to):
        return pltpu.make_async_remote_copy(
            src_ref=eout.at[to], dst_ref=ein.at[p_me],
            send_sem=es_sem, recv_sem=e_sem.at[p_me // 2],
            device_id=(gx_to[dx], to), device_id_type=MESH,
        )

    spare = jnp.ones((4, ROWS), F32)
    for dy in (2, 1, 3, 0):
        q = lax.rem(y_me + dy, NG // 2)
        for i in range(0, SUB, WIDE):
            dist = jnp.dot(
                book[q, i * CODES : (i + WIDE) * CODES, :], wt[q], preferred_element_type=F32
            )
            low = jnp.min(dist.reshape(WIDE, CODES, 256), axis=1)
            qmin[2 * q, i : i + WIDE, :] += low[:, :128]
            qmin[2 * q + 1, i : i + WIDE, :] += low[:, 128:]
        for c in range(2):
            eout[2 * q + c] = jnp.concatenate([qmin[2 * q + c, 0:SUB, :], spare], axis=0).astype(BF16)
        for dx in (2, 1, 3, 0):
            for c in range(2) if dx or dy else (0,):
                to = 2 * q + c if dx or dy else 2 * q + 1 - core
                err_copy(dx, to).start()
    ein[p_me] = eout[g]

    for j in range(NG):
        q_ref[j * SUB : (j + 1) * SUB, :] = qmin[j, 0:SUB, :]

    lax.fori_loop(0, NP // 2, places, 0)
    total = jnp.zeros((NZ * 16, 128), F32)
    for dx, dy in ARRIVAL:
        pp = lax.rem(x + dx, 4) * 4 + lax.rem(y_me + dy, 4)
        all_of(ein.at[0 : 2 if dx or dy else 1], e_sem.at[pp]).wait_recv()
        for h in range(2):
            err = ein[2 * pp + h].astype(F32)
            owner = zrow[pp, 0:1, h * 128 : (h + 1) * 128]
            for a in range(NZ):
                lm[pp, a * 16 : (a + 1) * 16, h * 128 : (h + 1) * 128] = jnp.where(
                    owner == float(a), err, 0.0
                ).astype(BF16)
        total = total + lax.dot_general(
            lm[pp], bt[pp], (((1,), (1,)), ((), ())), preferred_element_type=F32
        )
    lane8 = lax.broadcasted_iota(jnp.int32, (8, 128), 1)
    for a in range(NZ):
        pout[a] = jnp.where(
            lane8 < OWN, total[a * 16 : a * 16 + 8, :], total[a * 16 + 8 : a * 16 + 16, :]
        ).astype(BF16)

    def sum_copy(d):
        to = at_z(d)
        return pltpu.make_async_remote_copy(
            src_ref=pout.at[to], dst_ref=pin.at[z],
            send_sem=ps_sem, recv_sem=p_sem,
            device_id=(to * NX + x, g), device_id_type=MESH,
        )

    for d in (8, 7, 9, 6, 10, 5, 11, 4, 12, 3, 13, 2, 14, 1, 15):
        sum_copy(d).start()
    pin[z] = pout[z]
    for ref, sem in (
        (cg.at[0 : NZ - 1], zs_sem),
        (cg.at[0 : NZ * (NX - 1)], xs_sem),
        (cb.at[0 : NG - 1], cbs_sem),
        (slots.at[0 : NP - 1], sls_sem),
        (wout.at[0 : NG - 1], ws_sem),
        (ein.at[0 : NP - 1], es_sem),
    ):
        all_of(ref, sem).wait_send()

    all_of(pin.at[0 : NZ - 1], p_sem).wait_recv()
    whole = jnp.sum(pin[...].astype(F32), axis=0)
    count = jnp.broadcast_to(whole[4:5, :], (8, 128))
    count = jnp.where(lane8 < OWN, pltpu.roll(count, OWN, 1), count)
    mean = whole / jnp.maximum(count, 1.0)
    mean_ref[0:8, :] = mean[:, :OWN]
    mean_ref[8:SUB, :] = pltpu.roll(mean, OWN, 1)[: SUB - 8, :OWN]

    all_of(pout.at[0 : NZ - 1], ps_sem).wait_send()


def on_device(vectors, list_ids, old_order, new_order, centroids, rotation, codebook):
    dma = pltpu.SemaphoreType.DMA
    any_spec = pl.BlockSpec(memory_space=pltpu.HBM)
    errors, means = pl.pallas_call(
        kernel,
        out_shape=(
            jax.ShapeDtypeStruct((NG * SUB, ROWS), F32),
            jax.ShapeDtypeStruct((SUB, OWN), F32),
        ),
        in_specs=[any_spec] * 7,
        out_specs=(pl.BlockSpec(memory_space=pltpu.VMEM),) * 2,
        scratch_shapes=[
            pltpu.VMEM((ROWS, 768), BF16),
            pltpu.VMEM((1, 128), jnp.int32),
            pltpu.VMEM((32, 128), jnp.int32),
            pltpu.VMEM((32, 128), jnp.int32),
            pltpu.VMEM((OWN, FEAT), BF16),
            pltpu.VMEM((NZ * NX, PACKED, 128), BF16),
            pltpu.VMEM((768, 768), BF16),
            pltpu.VMEM((NG, SUB, 8, CODES), BF16),
            pltpu.VMEM((2, 128), F32),
            pltpu.VMEM((NP, 2, 128), F32),
            pltpu.VMEM((NG * ROWS, 128), F32),
            pltpu.VMEM((NG * ROWS, 256), BF16),
            pltpu.VMEM((128, CODES), F32),
            pltpu.VMEM((NG // 2, SUB * CODES, 256), BF16),
            pltpu.VMEM((NG // 2, 256, 256), BF16),
            pltpu.VMEM((NG * ROWS, 128), F32),
            pltpu.VMEM((NG, FEAT, 128), BF16),
            pltpu.VMEM((NG, FEAT, 128), BF16),
            pltpu.VMEM((ROWS, 768), F32),
            pltpu.VMEM((NG, 16, ROWS), F32),
            pltpu.VMEM((768, ROWS), F32),
            pltpu.VMEM((NG, 16, ROWS), BF16),
            pltpu.VMEM((NP, 16, ROWS), BF16),
            pltpu.VMEM((NP // 2, 8, 256), F32),
            pltpu.VMEM((NP // 2, 128, 256), BF16),
            pltpu.VMEM((NP // 2, NZ * 16, 256), BF16),
            pltpu.VMEM((NZ, 8, 128), BF16),
            pltpu.VMEM((NZ, 8, 128), BF16),
            dma((7,)),
            dma,
            dma,
            dma((NZ,)),
            dma((NZ // 2,)),
            dma,
            dma,
            dma,
            dma,
            dma,
            dma((NG // 2,)),
            dma,
            dma((NP // 2,)),
            dma,
            dma,
        ],
        compiler_params=pltpu.CompilerParams(
            collective_id=0, has_side_effects=True, vmem_limit_bytes=48 * 1024 * 1024
        ),
    )(
        *(
            pltpu.with_memory_space_constraint(one, pltpu.HBM)
            for one in (
                vectors,
                list_ids.reshape(1, ROWS),
                old_order.reshape(32, 128),
                new_order.reshape(32, 128),
                centroids,
                rotation,
                codebook,
            )
        )
    )
    return errors.T, means.T


def solution(mesh):
    both = ("gx", "gy")
    in_specs = (P(both, None), P(both), P(), P(), P("gx", "gy"), P(), P("gy", None, None))
    out_specs = (P(both, None), P("gx", "gy"))
    return jax.shard_map(
        on_device, mesh=mesh, in_specs=in_specs, out_specs=out_specs, check_vma=False
    )
```

```python
import jax
import jax.numpy as jnp
from jax import lax
from jax.experimental import pallas as pl
from jax.experimental.pallas import tpu as pltpu
from jax.sharding import PartitionSpec as P

MESH = pl.DeviceIdType.MESH
F32 = jnp.float32
BF16 = jnp.bfloat16

NZ, NX, NG = 16, 4, 8
NP = NX * NG
OWN = 64
FEAT = 96
SUB = 12
ROWS = 128
CODES = 256
CHUNK = 256
PACKED = OWN * FEAT // 128
WIDE = 6
HOP = 4
NEAR = [4, -4, 1, -1, 2, -2, 3, -3]
ARRIVAL = [
    (0, 0), (0, 2), (0, 3), (1, 2), (3, 2), (1, 3), (3, 3), (0, 1),
    (2, 2), (2, 3), (1, 1), (3, 1), (1, 0), (3, 0), (2, 1), (2, 0),
]
FAR = [5, -5, 6, -6, 7, -7, 8]
ORDER = [0, 1, -1, 2, -2, 3, -3, 4, -4] + FAR


def kernel(
    v_hbm, ids_hbm, old_hbm, new_hbm, c_hbm, r_hbm, cb_hbm,
    q_ref, mean_ref,
    v, ids, old, new, block_in, cg, rot, cb,
    slot_out, slots, high, low_hot, y, book, wt, acc, wout, win, vr,
    qmin, tt, eout, ein, zrow, bt, lm, pout, pin,
    in_sem, zs_sem, xs_sem, ag_sem, ax_sem, cbs_sem, cb_sem, sls_sem, sl_sem,
    ws_sem, w_sem, es_sem, e_sem, ps_sem, p_sem,
):
    gx, g = lax.axis_index("gx"), lax.axis_index("gy")
    z, x = gx // NX, gx % NX
    p_me = x * NG + g

    def at_z(off):
        return lax.rem(z + (off + NZ), NZ)

    x_to = [lax.rem(x + d, NX) for d in range(NX)]
    g_to = [lax.rem(g + d, NG) for d in range(NG)]
    gx_to = [z * NX + one for one in x_to]
    plane = [(dx, dg) for dx in (2, 1, 3, 0) for dg in (4, 5, 2, 3, 6, 7, 1, 0) if dx or dg]

    barrier = pltpu.get_barrier_semaphore()
    for off in NEAR:
        pl.semaphore_signal(barrier, inc=1, device_id=(at_z(off) * NX + x, g), device_id_type=MESH)

    for dx, dg in plane:
        pl.semaphore_signal(barrier, inc=1, device_id=(gx_to[dx], g_to[dg]), device_id_type=MESH)

    loads = [
        pltpu.make_async_copy(c_hbm, block_in, in_sem.at[0]),
        pltpu.make_async_copy(ids_hbm, ids, in_sem.at[1]),
        pltpu.make_async_copy(old_hbm, old, in_sem.at[2]),
        pltpu.make_async_copy(new_hbm, new, in_sem.at[3]),
        pltpu.make_async_copy(cb_hbm, cb.at[g], in_sem.at[4]),
        pltpu.make_async_copy(v_hbm, v, in_sem.at[5]),
        pltpu.make_async_copy(r_hbm, rot, in_sem.at[6]),
    ]
    for one in loads:
        one.start()

    loads[0].wait()
    for k in range(3):
        tail = block_in[48:64, 32 * k : 32 * (k + 1)]
        cg[gx, 16 * k : 16 * (k + 1), :] = jnp.concatenate(
            [block_in[16 * k : 16 * (k + 1), :], tail], axis=1
        )
    pl.semaphore_wait(barrier, len(NEAR) + NP - 1)

    def all_of(ref, sem):
        return pltpu.make_async_remote_copy(
            src_ref=ref, dst_ref=ref, send_sem=sem, recv_sem=sem,
            device_id=(gx, g), device_id_type=MESH,
        )

    def z_copy(block_z, to_off):
        block = block_z * NX + x
        return pltpu.make_async_remote_copy(
            src_ref=cg.at[block], dst_ref=cg.at[block],
            send_sem=zs_sem, recv_sem=ag_sem.at[block_z],
            device_id=(at_z(to_off) * NX + x, g), device_id_type=MESH,
        )

    def x_copy(off, d):
        block = at_z(off) * NX + x
        return pltpu.make_async_remote_copy(
            src_ref=cg.at[block], dst_ref=cg.at[block],
            send_sem=xs_sem, recv_sem=ax_sem.at[ORDER.index(off) // 2],
            device_id=(gx_to[d], g), device_id_type=MESH,
        )

    def got(off):
        all_of(cg.at[0], ag_sem.at[at_z(off)]).wait_recv()

    for off in NEAR:
        z_copy(z, off).start()
    for d in (1, 3, 2):
        x_copy(0, d).start()

    for k in (1, 2, 3):
        loads[k].wait()
    lane = lax.broadcasted_iota(jnp.int32, (ROWS, 128), 1)
    lane_f = lane.astype(F32)
    id_col = jnp.broadcast_to(ids[...].astype(F32), (ROWS, 128)).T

    def find(order, row):
        total = jnp.zeros((ROWS, 128), F32)
        for k in range(32):
            entry = jnp.broadcast_to(order[k : k + 1, :].astype(F32), (ROWS, 128))
            total = total + jnp.where(id_col == entry, lane_f + float(128 * k), 0.0)
        slot_out[row : row + 1, :] = jnp.sum(total.T, axis=0, keepdims=True)

    find(old, 0)
    find(new, 1)

    def slot_copy(dx, dg):
        return pltpu.make_async_remote_copy(
            src_ref=slot_out, dst_ref=slots.at[p_me],
            send_sem=sls_sem, recv_sem=sl_sem,
            device_id=(gx_to[dx], g_to[dg]), device_id_type=MESH,
        )

    for dx, dg in plane:
        slot_copy(dx, dg).start()
    slots[p_me] = slot_out[...]

    def book_copy(d):
        return pltpu.make_async_remote_copy(
            src_ref=cb.at[g], dst_ref=cb.at[g],
            send_sem=cbs_sem, recv_sem=cb_sem,
            device_id=(gx, lax.rem(g + d, NG)), device_id_type=MESH,
        )

    loads[4].wait()
    for d in range(1, NG):
        book_copy(d).start()

    loads[5].wait()
    loads[6].wait()
    vr[...] = jnp.dot(v[...], rot[...], preferred_element_type=F32)

    def spread(off):
        for d in (2, 1, 3):
            x_copy(off, d).start()

    for off in NEAR[2:6]:
        got(off)
        spread(off)
    for off in NEAR[:2]:
        got(off)
        step = -1 if off > 0 else 1
        for far in (1, 4, 3, 2) if off > 0 else (1, 3, 2):
            z_copy(at_z(off), step * far).start()
    for off in NEAR[6:] + NEAR[:2]:
        if abs(off) < HOP:
            got(off)
        spread(off)

    y[...] = jnp.zeros_like(y)
    wt[...] = jnp.zeros_like(wt)
    for q in range(NG // 2):
        for h in range(2):
            wt[q, h * 128 + FEAT : (h + 1) * 128, h * 128 : (h + 1) * 128] = jnp.ones((32, 128), BF16)

    lane_row = lax.broadcasted_iota(jnp.int32, (1, 128), 1)
    member = jnp.where(lane_row < FEAT, lane_row // 8, lax.rem(lane_row - FEAT, 16))

    def build_book(q, carry):
        for h in range(2):
            words = cb[2 * q + h].astype(F32)
            norm = jnp.sum(words * words, axis=1)
            high = norm.astype(BF16).astype(F32)
            y[0:FEAT, :] = -2.0 * words.reshape(FEAT, CODES)
            y[FEAT : FEAT + SUB, :] = high
            y[FEAT + 16 : FEAT + 16 + SUB, :] = (norm - high).astype(BF16).astype(F32)
            turned_words = y[...].T.astype(BF16)
            for i in range(SUB):
                mask = jnp.where(member == i, 1.0, 0.0).astype(BF16)
                book[q, i * CODES : (i + 1) * CODES, h * 128 : (h + 1) * 128] = turned_words * mask
        return carry


    all_of(slots.at[0 : NP - 1], sl_sem).wait_recv()

    def columns(j, carry):
        row = slots[x * NG + j][0:1, :].astype(jnp.int32)
        at = pl.ds(pl.multiple_of(j * ROWS, ROWS), ROWS)
        high[at, :] = jnp.broadcast_to((row // CHUNK).astype(F32), (ROWS, 128)).T
        inner = row % CHUNK
        block, spot = inner // OWN, inner % OWN
        place = jnp.where(spot < 48, block * 48 + spot, 144 + block * 16 + spot)
        rest = jnp.broadcast_to(place.astype(F32), (ROWS, 128)).T
        for h in range(2):
            low_hot[at, h * 128 : (h + 1) * 128] = jnp.where(
                rest == lane_f + float(128 * h), -1.0, 0.0
            ).astype(BF16)
        return carry

    lax.fori_loop(0, NG, columns, 0)
    local = lax.rem(lax.broadcasted_iota(jnp.int32, (128, 128), 0), OWN)

    def places(pp, carry):
        for h in range(2):
            at = slots[2 * pp + h][1:2, :].astype(jnp.int32)
            owner = at // OWN
            zrow[pp, :, h * 128 : (h + 1) * 128] = jnp.broadcast_to(
                jnp.where(owner % NX == x, (owner // NX).astype(F32), -1.0), (8, 128)
            )
            hit = jnp.broadcast_to(at % OWN, (128, 128)) == local
            bt[pp, :, h * 128 : (h + 1) * 128] = jnp.where(hit, 1.0, 0.0).astype(BF16)
        return carry

    acc[...] = jnp.zeros_like(acc)
    blank = jnp.zeros((16, 128 - FEAT), BF16)

    def operand(offs):
        all_of(cg.at[0:6], ax_sem.at[ORDER.index(offs[0]) // 2]).wait_recv()
        sides = []
        for off in offs:
            cz = at_z(off)
            blocks = [cg[cz * NX + b] for b in range(NX)]
            tails = [
                jnp.concatenate(
                    [one[16 * k : 16 * (k + 1), FEAT:] for k in range(3)] + [blank], axis=1
                )
                for one in blocks
            ]
            sides.append(jnp.concatenate(blocks + tails, axis=0))
        return jnp.concatenate(sides, axis=1)

    def choose(part, offs, hi, before):
        za, zb = (at_z(off).astype(F32) for off in offs)
        return jnp.where(hi == za, part[:, :128], jnp.where(hi == zb, part[:, 128:], before))

    def pick(offs):
        part = jnp.dot(low_hot[...], operand(offs), preferred_element_type=F32)
        acc[...] = choose(part, offs, high[...], acc[...])


    def pass_on(offs):
        for off in offs:
            got(off)
            spread(off)

    pick(ORDER[0:2])
    pass_on(FAR[0:2])
    pick(ORDER[2:4])
    pass_on(FAR[2:4])
    pick(ORDER[4:6])
    pass_on(FAR[4:])
    pick(ORDER[6:8])
    all_of(cb.at[0 : NG - 1], cb_sem).wait_recv()
    lax.fori_loop(0, NG // 4, build_book, 0)
    for k in range(NZ // 2, NZ - 2, 2):
        pick(ORDER[k : k + 2])

    def pick_copy(to):
        return pltpu.make_async_remote_copy(
            src_ref=wout.at[to], dst_ref=win.at[g],
            send_sem=ws_sem, recv_sem=w_sem.at[g // 2],
            device_id=(gx, to), device_id_type=MESH,
        )

    last = ORDER[NZ - 2 :]
    final = operand(last)
    y_me, core = g // 2, g % 2
    for dy in (2, 1, 3, 0):
        chip = lax.rem(y_me + dy, NG // 2)
        at = pl.ds(pl.multiple_of(chip * 2 * ROWS, 2 * ROWS), 2 * ROWS)
        part = jnp.dot(low_hot[at, :], final, preferred_element_type=F32)
        rows = choose(part, last, high[at, :], acc[at, :]).astype(BF16)
        for c in range(2):
            mine = rows[c * ROWS : (c + 1) * ROWS]
            for k in range(3):
                wout[2 * chip + c, 32 * k : 32 * (k + 1), :] = jnp.concatenate(
                    [mine[32 * k : 32 * (k + 1), :FEAT], mine[FEAT:, 32 * k : 32 * (k + 1)]], axis=1
                )
        if dy:
            for c in range(2):
                pick_copy(2 * chip + c).start()
        else:
            pick_copy(2 * chip + 1 - core).start()
    win[g] = wout[g]

    lax.fori_loop(NG // 4, NG // 2, build_book, 0)
    for dys in ((0,), (1,), (3, 2)):
        chips = [lax.rem(y_me + dy, NG // 2) for dy in dys]
        for dy, chip in zip(dys, chips):
            all_of(win.at[0 : 2 if dy else 1], w_sem.at[chip]).wait_recv()
        moved = None
        for chip in chips:
            sides = []
            for c in range(2):
                packed = win[2 * chip + c]
                tail = jnp.concatenate([packed[32 * k : 32 * (k + 1), FEAT:] for k in range(3)], axis=1)
                sides.append(jnp.concatenate([packed[:, :FEAT], tail], axis=0))
            part = jnp.dot(
                jnp.concatenate(sides, axis=1),
                rot[pl.ds(pl.multiple_of(chip * 2 * FEAT, 64), 2 * FEAT), :],
                preferred_element_type=F32,
            )
            moved = part if moved is None else moved + part
        vr[...] += moved
    tt[...] = vr[...].T
    for j in range(NG):
        q, h = j // 2, j % 2
        part = tt[j * FEAT : (j + 1) * FEAT, :]
        wt[q, h * 128 : h * 128 + FEAT, h * 128 : (h + 1) * 128] = part.astype(BF16)
        qmin[j, 0:SUB, :] = jnp.sum((part * part).reshape(SUB, 8, ROWS), axis=1)

    def err_copy(dx, to):
        return pltpu.make_async_remote_copy(
            src_ref=eout.at[to], dst_ref=ein.at[p_me],
            send_sem=es_sem, recv_sem=e_sem.at[p_me // 2],
            device_id=(gx_to[dx], to), device_id_type=MESH,
        )

    spare = jnp.ones((4, ROWS), F32)
    for dy in (2, 1, 3, 0):
        q = lax.rem(y_me + dy, NG // 2)
        for i in range(0, SUB, WIDE):
            dist = jnp.dot(
                book[q, i * CODES : (i + WIDE) * CODES, :], wt[q], preferred_element_type=F32
            )
            low = jnp.min(dist.reshape(WIDE, CODES, 256), axis=1)
            qmin[2 * q, i : i + WIDE, :] += low[:, :128]
            qmin[2 * q + 1, i : i + WIDE, :] += low[:, 128:]
        for c in range(2):
            eout[2 * q + c] = jnp.concatenate([qmin[2 * q + c, 0:SUB, :], spare], axis=0).astype(BF16)
        for dx in (2, 1, 3, 0):
            for c in range(2) if dx or dy else (0,):
                to = 2 * q + c if dx or dy else 2 * q + 1 - core
                err_copy(dx, to).start()
    ein[p_me] = eout[g]

    for j in range(NG):
        q_ref[j * SUB : (j + 1) * SUB, :] = qmin[j, 0:SUB, :]

    lax.fori_loop(0, NP // 2, places, 0)
    total = jnp.zeros((NZ * 16, 128), F32)
    for dx, dy in ARRIVAL:
        pp = lax.rem(x + dx, 4) * 4 + lax.rem(y_me + dy, 4)
        all_of(ein.at[0 : 2 if dx or dy else 1], e_sem.at[pp]).wait_recv()
        for h in range(2):
            err = ein[2 * pp + h].astype(F32)
            owner = zrow[pp, 0:1, h * 128 : (h + 1) * 128]
            for a in range(NZ):
                lm[pp, a * 16 : (a + 1) * 16, h * 128 : (h + 1) * 128] = jnp.where(
                    owner == float(a), err, 0.0
                ).astype(BF16)
        total = total + lax.dot_general(
            lm[pp], bt[pp], (((1,), (1,)), ((), ())), preferred_element_type=F32
        )
    lane8 = lax.broadcasted_iota(jnp.int32, (8, 128), 1)
    for a in range(NZ):
        pout[a] = jnp.where(
            lane8 < OWN, total[a * 16 : a * 16 + 8, :], total[a * 16 + 8 : a * 16 + 16, :]
        ).astype(BF16)

    def sum_copy(d):
        to = at_z(d)
        return pltpu.make_async_remote_copy(
            src_ref=pout.at[to], dst_ref=pin.at[z],
            send_sem=ps_sem, recv_sem=p_sem,
            device_id=(to * NX + x, g), device_id_type=MESH,
        )

    for d in (8, 7, 9, 6, 10, 5, 11, 4, 12, 3, 13, 2, 14, 1, 15):
        sum_copy(d).start()
    pin[z] = pout[z]
    for ref, sem in (
        (cg.at[0 : NZ - 1], zs_sem),
        (cg.at[0 : NZ * (NX - 1)], xs_sem),
        (cb.at[0 : NG - 1], cbs_sem),
        (slots.at[0 : NP - 1], sls_sem),
        (wout.at[0 : NG - 1], ws_sem),
        (ein.at[0 : NP - 1], es_sem),
    ):
        all_of(ref, sem).wait_send()

    all_of(pin.at[0 : NZ - 1], p_sem).wait_recv()
    whole = jnp.sum(pin[...].astype(F32), axis=0)
    count = jnp.broadcast_to(whole[4:5, :], (8, 128))
    count = jnp.where(lane8 < OWN, pltpu.roll(count, OWN, 1), count)
    mean = whole / jnp.maximum(count, 1.0)
    mean_ref[0:8, :] = mean[:, :OWN]
    mean_ref[8:SUB, :] = pltpu.roll(mean, OWN, 1)[: SUB - 8, :OWN]

    all_of(pout.at[0 : NZ - 1], ps_sem).wait_send()


def put_out(q_in, mean_in, q_out, mean_out, q_sem, mean_sem):
    copies = [
        pltpu.make_async_copy(q_in, q_out, q_sem),
        pltpu.make_async_copy(mean_in, mean_out, mean_sem),
    ]
    for one in copies:
        one.start()
    for one in copies:
        one.wait()


def on_device(vectors, list_ids, old_order, new_order, centroids, rotation, codebook):
    dma = pltpu.SemaphoreType.DMA
    any_spec = pl.BlockSpec(memory_space=pltpu.HBM)
    found = pl.pallas_call(
        kernel,
        out_shape=(
            jax.ShapeDtypeStruct((NG * SUB, ROWS), F32),
            jax.ShapeDtypeStruct((SUB, OWN), F32),
        ),
        in_specs=[any_spec] * 7,
        out_specs=(pl.BlockSpec(memory_space=pltpu.VMEM),) * 2,
        scratch_shapes=[
            pltpu.VMEM((ROWS, 768), BF16),
            pltpu.VMEM((1, 128), jnp.int32),
            pltpu.VMEM((32, 128), jnp.int32),
            pltpu.VMEM((32, 128), jnp.int32),
            pltpu.VMEM((OWN, FEAT), BF16),
            pltpu.VMEM((NZ * NX, PACKED, 128), BF16),
            pltpu.VMEM((768, 768), BF16),
            pltpu.VMEM((NG, SUB, 8, CODES), BF16),
            pltpu.VMEM((2, 128), F32),
            pltpu.VMEM((NP, 2, 128), F32),
            pltpu.VMEM((NG * ROWS, 128), F32),
            pltpu.VMEM((NG * ROWS, 256), BF16),
            pltpu.VMEM((128, CODES), F32),
            pltpu.VMEM((NG // 2, SUB * CODES, 256), BF16),
            pltpu.VMEM((NG // 2, 256, 256), BF16),
            pltpu.VMEM((NG * ROWS, 128), F32),
            pltpu.VMEM((NG, FEAT, 128), BF16),
            pltpu.VMEM((NG, FEAT, 128), BF16),
            pltpu.VMEM((ROWS, 768), F32),
            pltpu.VMEM((NG, 16, ROWS), F32),
            pltpu.VMEM((768, ROWS), F32),
            pltpu.VMEM((NG, 16, ROWS), BF16),
            pltpu.VMEM((NP, 16, ROWS), BF16),
            pltpu.VMEM((NP // 2, 8, 256), F32),
            pltpu.VMEM((NP // 2, 128, 256), BF16),
            pltpu.VMEM((NP // 2, NZ * 16, 256), BF16),
            pltpu.VMEM((NZ, 8, 128), BF16),
            pltpu.VMEM((NZ, 8, 128), BF16),
            dma((7,)),
            dma,
            dma,
            dma((NZ,)),
            dma((NZ // 2,)),
            dma,
            dma,
            dma,
            dma,
            dma,
            dma((NG // 2,)),
            dma,
            dma((NP // 2,)),
            dma,
            dma,
        ],
        compiler_params=pltpu.CompilerParams(
            collective_id=0, has_side_effects=True, vmem_limit_bytes=48 * 1024 * 1024
        ),
    )(
        *(
            pltpu.with_memory_space_constraint(one, pltpu.HBM)
            for one in (
                vectors,
                list_ids.reshape(1, ROWS),
                old_order.reshape(32, 128),
                new_order.reshape(32, 128),
                centroids,
                rotation,
                codebook,
            )
        )
    )
    errors, means = pl.pallas_call(
        put_out,
        out_shape=(
            jax.ShapeDtypeStruct((NG * SUB, ROWS), F32),
            jax.ShapeDtypeStruct((SUB, OWN), F32),
        ),
        in_specs=[pl.BlockSpec(memory_space=pltpu.VMEM)] * 2,
        out_specs=(any_spec, any_spec),
        scratch_shapes=[dma, dma],
    )(*(pltpu.with_memory_space_constraint(one, pltpu.VMEM) for one in found))
    return errors.T, means.T


def solution(mesh):
    both = ("gx", "gy")
    in_specs = (P(both, None), P(both), P(), P(), P("gx", "gy"), P(), P("gy", None, None))
    out_specs = (P(both, None), P("gx", "gy"))
    return jax.shard_map(
        on_device, mesh=mesh, in_specs=in_specs, out_specs=out_specs, check_vma=False
    )
```

```python
import jax
import jax.numpy as jnp
from jax import lax
from jax.experimental import pallas as pl
from jax.experimental.pallas import tpu as pltpu
from jax.sharding import PartitionSpec as P

MESH = pl.DeviceIdType.MESH
F32 = jnp.float32
BF16 = jnp.bfloat16

NZ, NX, NG = 16, 4, 8
NP = NX * NG
OWN = 64
FEAT = 96
SUB = 12
ROWS = 128
CODES = 256
CHUNK = 256
PACKED = OWN * FEAT // 128
WIDE = 6
HOP = 4
NEAR = [4, -4, 1, -1, 2, -2, 3, -3]
ARRIVAL = [
    (0, 0), (0, 2), (0, 3), (1, 2), (3, 2), (1, 3), (3, 3), (0, 1),
    (2, 2), (2, 3), (1, 1), (3, 1), (1, 0), (3, 0), (2, 1), (2, 0),
]
FAR = [5, -5, 6, -6, 7, -7, 8]
ORDER = [0, 1, -1, 2, -2, 3, -3, 4, -4] + FAR


def kernel(
    v_hbm, ids_hbm, old_hbm, new_hbm, c_hbm, r_hbm, cb_hbm,
    q_ref, mean_ref,
    v, ids, old, new, block_in, cg, rot, cb,
    slot_out, slots, high, low_hot, y, book, wt, acc, wout, win, vr,
    qmin, tt, eout, ein, zrow, bt, lm, pout, pin,
    in_sem, zs_sem, xs_sem, ag_sem, ax_sem, cbs_sem, cb_sem, sls_sem, sl_sem, slx_sem,
    ws_sem, w_sem, es_sem, e_sem, ps_sem, p_sem,
):
    gx, g = lax.axis_index("gx"), lax.axis_index("gy")
    z, x = gx // NX, gx % NX
    p_me = x * NG + g

    def at_z(off):
        return lax.rem(z + (off + NZ), NZ)

    x_to = [lax.rem(x + d, NX) for d in range(NX)]
    g_to = [lax.rem(g + d, NG) for d in range(NG)]
    gx_to = [z * NX + one for one in x_to]
    plane = [(dx, dg) for dx in (2, 1, 3, 0) for dg in (4, 5, 2, 3, 6, 7, 1, 0) if dx or dg]

    barrier = pltpu.get_barrier_semaphore()
    for off in NEAR:
        pl.semaphore_signal(barrier, inc=1, device_id=(at_z(off) * NX + x, g), device_id_type=MESH)

    beside = [(dx, dg) for dx, dg in plane if dx == 0 or dg == 0]
    for dx, dg in beside:
        pl.semaphore_signal(barrier, inc=1, device_id=(gx_to[dx], g_to[dg]), device_id_type=MESH)

    loads = [
        pltpu.make_async_copy(c_hbm, block_in, in_sem.at[0]),
        pltpu.make_async_copy(ids_hbm, ids, in_sem.at[1]),
        pltpu.make_async_copy(old_hbm, old, in_sem.at[2]),
        pltpu.make_async_copy(new_hbm, new, in_sem.at[3]),
        pltpu.make_async_copy(cb_hbm, cb.at[g], in_sem.at[4]),
        pltpu.make_async_copy(v_hbm, v, in_sem.at[5]),
        pltpu.make_async_copy(r_hbm, rot, in_sem.at[6]),
    ]
    for one in loads:
        one.start()

    loads[0].wait()
    for k in range(3):
        tail = block_in[48:64, 32 * k : 32 * (k + 1)]
        cg[gx, 16 * k : 16 * (k + 1), :] = jnp.concatenate(
            [block_in[16 * k : 16 * (k + 1), :], tail], axis=1
        )
    pl.semaphore_wait(barrier, len(NEAR) + len(beside))

    def all_of(ref, sem):
        return pltpu.make_async_remote_copy(
            src_ref=ref, dst_ref=ref, send_sem=sem, recv_sem=sem,
            device_id=(gx, g), device_id_type=MESH,
        )

    def z_copy(block_z, to_off):
        block = block_z * NX + x
        return pltpu.make_async_remote_copy(
            src_ref=cg.at[block], dst_ref=cg.at[block],
            send_sem=zs_sem, recv_sem=ag_sem.at[block_z],
            device_id=(at_z(to_off) * NX + x, g), device_id_type=MESH,
        )

    def x_copy(off, d):
        block = at_z(off) * NX + x
        return pltpu.make_async_remote_copy(
            src_ref=cg.at[block], dst_ref=cg.at[block],
            send_sem=xs_sem, recv_sem=ax_sem.at[ORDER.index(off) // 2],
            device_id=(gx_to[d], g), device_id_type=MESH,
        )

    def got(off):
        all_of(cg.at[0], ag_sem.at[at_z(off)]).wait_recv()

    for off in NEAR:
        z_copy(z, off).start()
    for d in (1, 3, 2):
        x_copy(0, d).start()

    for k in (1, 2, 3):
        loads[k].wait()
    lane = lax.broadcasted_iota(jnp.int32, (ROWS, 128), 1)
    lane_f = lane.astype(F32)
    id_col = jnp.broadcast_to(ids[...].astype(F32), (ROWS, 128)).T

    def find(order, row):
        total = jnp.zeros((ROWS, 128), F32)
        for k in range(32):
            entry = jnp.broadcast_to(order[k : k + 1, :].astype(F32), (ROWS, 128))
            total = total + jnp.where(id_col == entry, lane_f + float(128 * k), 0.0)
        slot_out[row : row + 1, :] = jnp.sum(total.T, axis=0, keepdims=True)

    find(old, 0)
    find(new, 1)

    def slot_copy(dx, dg):
        return pltpu.make_async_remote_copy(
            src_ref=slot_out, dst_ref=slots.at[p_me],
            send_sem=sls_sem, recv_sem=slx_sem if dx else sl_sem,
            device_id=(gx_to[dx], g_to[dg]), device_id_type=MESH,
        )

    for dx, dg in plane:
        if dx == 0:
            slot_copy(dx, dg).start()
    slots[p_me] = slot_out[...]

    def book_copy(d):
        return pltpu.make_async_remote_copy(
            src_ref=cb.at[g], dst_ref=cb.at[g],
            send_sem=cbs_sem, recv_sem=cb_sem,
            device_id=(gx, lax.rem(g + d, NG)), device_id_type=MESH,
        )

    loads[4].wait()
    for d in range(1, NG):
        book_copy(d).start()

    loads[5].wait()
    loads[6].wait()
    vr[...] = jnp.dot(v[...], rot[...], preferred_element_type=F32)

    def spread(off):
        for d in (2, 1, 3):
            x_copy(off, d).start()

    for off in NEAR[2:6]:
        got(off)
        spread(off)
    for off in NEAR[:2]:
        got(off)
        step = -1 if off > 0 else 1
        for far in (1, 4, 3, 2) if off > 0 else (1, 3, 2):
            z_copy(at_z(off), step * far).start()
    for off in NEAR[6:] + NEAR[:2]:
        if abs(off) < HOP:
            got(off)
        spread(off)

    y[...] = jnp.zeros_like(y)
    wt[...] = jnp.zeros_like(wt)
    for q in range(NG // 2):
        for h in range(2):
            wt[q, h * 128 + FEAT : (h + 1) * 128, h * 128 : (h + 1) * 128] = jnp.ones((32, 128), BF16)

    lane_row = lax.broadcasted_iota(jnp.int32, (1, 128), 1)
    member = jnp.where(lane_row < FEAT, lane_row // 8, lax.rem(lane_row - FEAT, 16))

    def build_book(q, carry):
        for h in range(2):
            words = cb[2 * q + h].astype(F32)
            norm = jnp.sum(words * words, axis=1)
            high = norm.astype(BF16).astype(F32)
            y[0:FEAT, :] = -2.0 * words.reshape(FEAT, CODES)
            y[FEAT : FEAT + SUB, :] = high
            y[FEAT + 16 : FEAT + 16 + SUB, :] = (norm - high).astype(BF16).astype(F32)
            turned_words = y[...].T.astype(BF16)
            for i in range(SUB):
                mask = jnp.where(member == i, 1.0, 0.0).astype(BF16)
                book[q, i * CODES : (i + 1) * CODES, h * 128 : (h + 1) * 128] = turned_words * mask
        return carry


    all_of(slots.at[0 : NG - 1], sl_sem).wait_recv()

    def columns(j, carry):
        row = slots[x * NG + j][0:1, :].astype(jnp.int32)
        at = pl.ds(pl.multiple_of(j * ROWS, ROWS), ROWS)
        high[at, :] = jnp.broadcast_to((row // CHUNK).astype(F32), (ROWS, 128)).T
        inner = row % CHUNK
        block, spot = inner // OWN, inner % OWN
        place = jnp.where(spot < 48, block * 48 + spot, 144 + block * 16 + spot)
        rest = jnp.broadcast_to(place.astype(F32), (ROWS, 128)).T
        for h in range(2):
            low_hot[at, h * 128 : (h + 1) * 128] = jnp.where(
                rest == lane_f + float(128 * h), -1.0, 0.0
            ).astype(BF16)
        return carry

    lax.fori_loop(0, NG, columns, 0)
    local = lax.rem(lax.broadcasted_iota(jnp.int32, (128, 128), 0), OWN)

    def places(pp, carry):
        for h in range(2):
            at = slots[2 * pp + h][1:2, :].astype(jnp.int32)
            owner = at // OWN
            zrow[pp, :, h * 128 : (h + 1) * 128] = jnp.broadcast_to(
                jnp.where(owner % NX == x, (owner // NX).astype(F32), -1.0), (8, 128)
            )
            hit = jnp.broadcast_to(at % OWN, (128, 128)) == local
            bt[pp, :, h * 128 : (h + 1) * 128] = jnp.where(hit, 1.0, 0.0).astype(BF16)
        return carry

    acc[...] = jnp.zeros_like(acc)
    blank = jnp.zeros((16, 128 - FEAT), BF16)

    def operand(offs):
        all_of(cg.at[0:6], ax_sem.at[ORDER.index(offs[0]) // 2]).wait_recv()
        sides = []
        for off in offs:
            cz = at_z(off)
            blocks = [cg[cz * NX + b] for b in range(NX)]
            tails = [
                jnp.concatenate(
                    [one[16 * k : 16 * (k + 1), FEAT:] for k in range(3)] + [blank], axis=1
                )
                for one in blocks
            ]
            sides.append(jnp.concatenate(blocks + tails, axis=0))
        return jnp.concatenate(sides, axis=1)

    def choose(part, offs, hi, before):
        za, zb = (at_z(off).astype(F32) for off in offs)
        return jnp.where(hi == za, part[:, :128], jnp.where(hi == zb, part[:, 128:], before))

    def pick(offs):
        part = jnp.dot(low_hot[...], operand(offs), preferred_element_type=F32)
        acc[...] = choose(part, offs, high[...], acc[...])


    def pass_on(offs):
        for off in offs:
            got(off)
            spread(off)

    pick(ORDER[0:2])
    for dx, dg in plane:
        if dx:
            slot_copy(dx, dg).start()
    pass_on(FAR[0:2])
    pick(ORDER[2:4])
    pass_on(FAR[2:4])
    pick(ORDER[4:6])
    pass_on(FAR[4:])
    pick(ORDER[6:8])
    all_of(cb.at[0 : NG - 1], cb_sem).wait_recv()
    lax.fori_loop(0, NG // 4, build_book, 0)
    for k in range(NZ // 2, NZ - 2, 2):
        pick(ORDER[k : k + 2])

    def pick_copy(to):
        return pltpu.make_async_remote_copy(
            src_ref=wout.at[to], dst_ref=win.at[g],
            send_sem=ws_sem, recv_sem=w_sem.at[g // 2],
            device_id=(gx, to), device_id_type=MESH,
        )

    last = ORDER[NZ - 2 :]
    final = operand(last)
    y_me, core = g // 2, g % 2
    for dy in (2, 1, 3, 0):
        chip = lax.rem(y_me + dy, NG // 2)
        at = pl.ds(pl.multiple_of(chip * 2 * ROWS, 2 * ROWS), 2 * ROWS)
        part = jnp.dot(low_hot[at, :], final, preferred_element_type=F32)
        rows = choose(part, last, high[at, :], acc[at, :]).astype(BF16)
        for c in range(2):
            mine = rows[c * ROWS : (c + 1) * ROWS]
            for k in range(3):
                wout[2 * chip + c, 32 * k : 32 * (k + 1), :] = jnp.concatenate(
                    [mine[32 * k : 32 * (k + 1), :FEAT], mine[FEAT:, 32 * k : 32 * (k + 1)]], axis=1
                )
        if dy:
            for c in range(2):
                pick_copy(2 * chip + c).start()
        else:
            pick_copy(2 * chip + 1 - core).start()
    win[g] = wout[g]

    lax.fori_loop(NG // 4, NG // 2, build_book, 0)
    for dys in ((0,), (1,), (3, 2)):
        chips = [lax.rem(y_me + dy, NG // 2) for dy in dys]
        for dy, chip in zip(dys, chips):
            all_of(win.at[0 : 2 if dy else 1], w_sem.at[chip]).wait_recv()
        moved = None
        for chip in chips:
            sides = []
            for c in range(2):
                packed = win[2 * chip + c]
                tail = jnp.concatenate([packed[32 * k : 32 * (k + 1), FEAT:] for k in range(3)], axis=1)
                sides.append(jnp.concatenate([packed[:, :FEAT], tail], axis=0))
            part = jnp.dot(
                jnp.concatenate(sides, axis=1),
                rot[pl.ds(pl.multiple_of(chip * 2 * FEAT, 64), 2 * FEAT), :],
                preferred_element_type=F32,
            )
            moved = part if moved is None else moved + part
        vr[...] += moved
    tt[...] = vr[...].T
    for j in range(NG):
        q, h = j // 2, j % 2
        part = tt[j * FEAT : (j + 1) * FEAT, :]
        wt[q, h * 128 : h * 128 + FEAT, h * 128 : (h + 1) * 128] = part.astype(BF16)
        qmin[j, 0:SUB, :] = jnp.sum((part * part).reshape(SUB, 8, ROWS), axis=1)

    def err_copy(dx, to):
        return pltpu.make_async_remote_copy(
            src_ref=eout.at[to], dst_ref=ein.at[p_me],
            send_sem=es_sem, recv_sem=e_sem.at[p_me // 2],
            device_id=(gx_to[dx], to), device_id_type=MESH,
        )

    spare = jnp.ones((4, ROWS), F32)
    for dy in (2, 1, 3, 0):
        q = lax.rem(y_me + dy, NG // 2)
        for i in range(0, SUB, WIDE):
            dist = jnp.dot(
                book[q, i * CODES : (i + WIDE) * CODES, :], wt[q], preferred_element_type=F32
            )
            low = jnp.min(dist.reshape(WIDE, CODES, 256), axis=1)
            qmin[2 * q, i : i + WIDE, :] += low[:, :128]
            qmin[2 * q + 1, i : i + WIDE, :] += low[:, 128:]
        for c in range(2):
            eout[2 * q + c] = jnp.concatenate([qmin[2 * q + c, 0:SUB, :], spare], axis=0).astype(BF16)
        for dx in (2, 1, 3, 0):
            for c in range(2) if dx or dy else (0,):
                to = 2 * q + c if dx or dy else 2 * q + 1 - core
                err_copy(dx, to).start()
    ein[p_me] = eout[g]

    for j in range(NG):
        q_ref[j * SUB : (j + 1) * SUB, :] = qmin[j, 0:SUB, :]

    all_of(slots.at[0 : NP - NG], slx_sem).wait_recv()
    lax.fori_loop(0, NP // 2, places, 0)
    total = jnp.zeros((NZ * 16, 128), F32)
    for dx, dy in ARRIVAL:
        pp = lax.rem(x + dx, 4) * 4 + lax.rem(y_me + dy, 4)
        all_of(ein.at[0 : 2 if dx or dy else 1], e_sem.at[pp]).wait_recv()
        for h in range(2):
            err = ein[2 * pp + h].astype(F32)
            owner = zrow[pp, 0:1, h * 128 : (h + 1) * 128]
            for a in range(NZ):
                lm[pp, a * 16 : (a + 1) * 16, h * 128 : (h + 1) * 128] = jnp.where(
                    owner == float(a), err, 0.0
                ).astype(BF16)
        total = total + lax.dot_general(
            lm[pp], bt[pp], (((1,), (1,)), ((), ())), preferred_element_type=F32
        )
    lane8 = lax.broadcasted_iota(jnp.int32, (8, 128), 1)
    for a in range(NZ):
        pout[a] = jnp.where(
            lane8 < OWN, total[a * 16 : a * 16 + 8, :], total[a * 16 + 8 : a * 16 + 16, :]
        ).astype(BF16)

    def sum_copy(d):
        to = at_z(d)
        return pltpu.make_async_remote_copy(
            src_ref=pout.at[to], dst_ref=pin.at[z],
            send_sem=ps_sem, recv_sem=p_sem,
            device_id=(to * NX + x, g), device_id_type=MESH,
        )

    for d in (8, 7, 9, 6, 10, 5, 11, 4, 12, 3, 13, 2, 14, 1, 15):
        sum_copy(d).start()
    pin[z] = pout[z]
    for ref, sem in (
        (cg.at[0 : NZ - 1], zs_sem),
        (cg.at[0 : NZ * (NX - 1)], xs_sem),
        (cb.at[0 : NG - 1], cbs_sem),
        (slots.at[0 : NP - 1], sls_sem),
        (wout.at[0 : NG - 1], ws_sem),
        (ein.at[0 : NP - 1], es_sem),
    ):
        all_of(ref, sem).wait_send()

    all_of(pin.at[0 : NZ - 1], p_sem).wait_recv()
    whole = jnp.sum(pin[...].astype(F32), axis=0)
    count = jnp.broadcast_to(whole[4:5, :], (8, 128))
    count = jnp.where(lane8 < OWN, pltpu.roll(count, OWN, 1), count)
    mean = whole / jnp.maximum(count, 1.0)
    mean_ref[0:8, :] = mean[:, :OWN]
    mean_ref[8:SUB, :] = pltpu.roll(mean, OWN, 1)[: SUB - 8, :OWN]

    all_of(pout.at[0 : NZ - 1], ps_sem).wait_send()


def put_out(q_in, mean_in, q_out, mean_out, q_sem, mean_sem):
    copies = [
        pltpu.make_async_copy(q_in, q_out, q_sem),
        pltpu.make_async_copy(mean_in, mean_out, mean_sem),
    ]
    for one in copies:
        one.start()
    for one in copies:
        one.wait()


def on_device(vectors, list_ids, old_order, new_order, centroids, rotation, codebook):
    dma = pltpu.SemaphoreType.DMA
    any_spec = pl.BlockSpec(memory_space=pltpu.HBM)
    found = pl.pallas_call(
        kernel,
        out_shape=(
            jax.ShapeDtypeStruct((NG * SUB, ROWS), F32),
            jax.ShapeDtypeStruct((SUB, OWN), F32),
        ),
        in_specs=[any_spec] * 7,
        out_specs=(pl.BlockSpec(memory_space=pltpu.VMEM),) * 2,
        scratch_shapes=[
            pltpu.VMEM((ROWS, 768), BF16),
            pltpu.VMEM((1, 128), jnp.int32),
            pltpu.VMEM((32, 128), jnp.int32),
            pltpu.VMEM((32, 128), jnp.int32),
            pltpu.VMEM((OWN, FEAT), BF16),
            pltpu.VMEM((NZ * NX, PACKED, 128), BF16),
            pltpu.VMEM((768, 768), BF16),
            pltpu.VMEM((NG, SUB, 8, CODES), BF16),
            pltpu.VMEM((2, 128), F32),
            pltpu.VMEM((NP, 2, 128), F32),
            pltpu.VMEM((NG * ROWS, 128), F32),
            pltpu.VMEM((NG * ROWS, 256), BF16),
            pltpu.VMEM((128, CODES), F32),
            pltpu.VMEM((NG // 2, SUB * CODES, 256), BF16),
            pltpu.VMEM((NG // 2, 256, 256), BF16),
            pltpu.VMEM((NG * ROWS, 128), F32),
            pltpu.VMEM((NG, FEAT, 128), BF16),
            pltpu.VMEM((NG, FEAT, 128), BF16),
            pltpu.VMEM((ROWS, 768), F32),
            pltpu.VMEM((NG, 16, ROWS), F32),
            pltpu.VMEM((768, ROWS), F32),
            pltpu.VMEM((NG, 16, ROWS), BF16),
            pltpu.VMEM((NP, 16, ROWS), BF16),
            pltpu.VMEM((NP // 2, 8, 256), F32),
            pltpu.VMEM((NP // 2, 128, 256), BF16),
            pltpu.VMEM((NP // 2, NZ * 16, 256), BF16),
            pltpu.VMEM((NZ, 8, 128), BF16),
            pltpu.VMEM((NZ, 8, 128), BF16),
            dma((7,)),
            dma,
            dma,
            dma((NZ,)),
            dma((NZ // 2,)),
            dma,
            dma,
            dma,
            dma,
            dma,
            dma,
            dma((NG // 2,)),
            dma,
            dma((NP // 2,)),
            dma,
            dma,
        ],
        compiler_params=pltpu.CompilerParams(
            collective_id=0, has_side_effects=True, vmem_limit_bytes=48 * 1024 * 1024
        ),
    )(
        *(
            pltpu.with_memory_space_constraint(one, pltpu.HBM)
            for one in (
                vectors,
                list_ids.reshape(1, ROWS),
                old_order.reshape(32, 128),
                new_order.reshape(32, 128),
                centroids,
                rotation,
                codebook,
            )
        )
    )
    errors, means = pl.pallas_call(
        put_out,
        out_shape=(
            jax.ShapeDtypeStruct((NG * SUB, ROWS), F32),
            jax.ShapeDtypeStruct((SUB, OWN), F32),
        ),
        in_specs=[pl.BlockSpec(memory_space=pltpu.VMEM)] * 2,
        out_specs=(any_spec, any_spec),
        scratch_shapes=[dma, dma],
    )(*(pltpu.with_memory_space_constraint(one, pltpu.VMEM) for one in found))
    return errors.T, means.T


def solution(mesh):
    both = ("gx", "gy")
    in_specs = (P(both, None), P(both), P(), P(), P("gx", "gy"), P(), P("gy", None, None))
    out_specs = (P(both, None), P("gx", "gy"))
    return jax.shard_map(
        on_device, mesh=mesh, in_specs=in_specs, out_specs=out_specs, check_vma=False
    )
```
